128 devices in a mesh: neg: 16 (over x, y), qry: 8 (over z, core).
Axes of the slice: x: 4, y: 4, z: 4, core: 2. Of those that a mesh axis runs over, the one named last changes fastest.
Arguments:
- items_table: bfloat16 [131072, 512], P('neg'), may hold values from -6 to 6
- fetch_rows: int32 [2048, 640], P(('neg', 'qry')), may hold values from 0 to 8191, as said below
- neighbour_slots: int32 [65536, 40], P(('neg', 'qry')), may hold values from 0 to 10239, as said below
- neighbour_count: int32 [65536], P(('neg', 'qry')), may hold values from 20 to 40
- self_slot: int32 [65536], P(('neg', 'qry')), may hold values from 0 to 10239
- negative_count: int32 [65536], P('neg'), may hold values from 1 to 999
- message_weight: bfloat16 [512, 512], replicated, may hold values from -0.25 to 0.25
- message_bias: float32 [512], replicated, may hold values from -3 to 3
- self_weight: bfloat16 [512, 512], replicated, may hold values from -0.25 to 0.25
- neighbour_weight: bfloat16 [512, 512], replicated, may hold values from -0.25 to 0.25
- output_bias: float32 [512], replicated, may hold values from -3 to 3
- queries: bfloat16 [8192, 512], P('qry'), may hold values from -8 to 8
Outputs:
- negative_embed: bfloat16 [65536, 512], P(('neg', 'qry'))
- query_lse: float32 [8192], P('qry')
The draws below stay inside these ranges and needn't reach their ends.
Inputs may be any that keep to these rules, and one draw needn't show every extreme that they name: Within one row of fetch_rows (one device's list for one partition) no item appears twice. `neighbour_slots`: every one of a device's 16 * 640 fetched rows is named by at least one live neighbour of that device's negatives.
All inputs are finite; a program needn't handle non-finite values.
Results may differ from the reference program's by a relative error of at most 0.0055.
Values may be sent and summed in bfloat16 or wider, within the bound.
A program may use at most 128 MiB of HBM per device.

```python
import math
import jax
import jax.numpy as jnp
from jax import lax

D = 512
K = 40
ITEM_DEV = 8192
NEG_DEV = 512
CAP = 640
NEG = 65536
QRY = 8192
ITEMS = 131072
N_NEG = 16
N_QRY = 8


def draw_queries(key, part):
    values = jnp.clip(jax.random.normal(key, (QRY, D), jnp.float32), -5.5, 5.5)
    return values.astype(jnp.bfloat16)


def draw_fetch_rows(key, part):
    row_keys = jax.random.split(jax.random.fold_in(key, 7), N_NEG * N_QRY * N_NEG)

    def one_row(row_key):
        return jax.random.permutation(row_key, ITEM_DEV)[:CAP].astype(jnp.int32)
    return jax.vmap(one_row)(row_keys).astype(jnp.int32)


def neighbour_draw(key):
    count_key = jax.random.fold_in(key, 11)
    counts = jax.random.randint(count_key, (NEG,), K // 2, K + 1, dtype=jnp.int32)
    slot_total = N_NEG * CAP
    device_keys = jax.random.split(jax.random.fold_in(key, 13), N_NEG * N_QRY)
    count_blocks = counts.reshape(N_NEG * N_QRY, NEG_DEV)

    def one_device(device_key, count_block):
        order_key = jax.random.fold_in(device_key, 1)
        filler_key = jax.random.fold_in(device_key, 2)
        live_mask = jnp.arange(K, dtype=jnp.int32)[None, :] < count_block[:, None]
        priority = jax.random.randint(order_key, (NEG_DEV * K,), 0, 1 << 20, dtype=jnp.int32)
        priority = priority + jnp.where(live_mask.reshape(-1), 0, 1 << 21).astype(jnp.int32)
        order = jnp.argsort(priority, stable=True).astype(jnp.int32)
        ranked = jnp.argsort(order, stable=True).astype(jnp.int32)
        filler = jax.random.randint(filler_key, (NEG_DEV * K,), 0, slot_total, dtype=jnp.int32)
        slots = jnp.where(ranked < slot_total, ranked, filler)
        return slots.reshape(NEG_DEV, K).astype(jnp.int32)
    slots = jax.vmap(one_device)(device_keys, count_blocks).reshape(NEG, K)
    return (counts, slots)


def draw_neighbour_count(key, part):
    return neighbour_draw(key)[0].astype(jnp.int32)


def draw_neighbour_slots(key, part):
    return neighbour_draw(key)[1].astype(jnp.int32)


def place_ends(drawn, stream_key, smallest, largest):
    longest = drawn.shape.index(max(drawn.shape))
    spots = []
    for shift in (0, 1):
        where = [jax.random.randint(jax.random.fold_in(stream_key, axis), (), 0, length) for axis, length in enumerate(drawn.shape)]
        where[longest] = (where[longest] + shift) % drawn.shape[longest]
        spots.append(tuple(where))
    return drawn.at[spots[0]].set(smallest).at[spots[1]].set(largest)


def shard_levels(own_key, shape, cuts, least, high):
    factor_of = 1.0
    for dim, parts in cuts:
        draws = jax.random.uniform(jax.random.fold_in(jax.random.fold_in(own_key, 6), dim), (parts,), jnp.float32, least / len(cuts), high / len(cuts))
        factor_of = factor_of * jnp.repeat(jnp.exp(draws), shape[dim] // parts).reshape((-1,) + (1,) * (len(shape) - 1 - dim))
    return factor_of


def gaussian(key, shape, deviation, limit, pieces=(), kind=jnp.bfloat16):
    factor_of = shard_levels(key, shape, pieces, -0.22, 0.18) if pieces else 1.0
    values = jax.random.normal(key, shape, jnp.float32) * deviation * factor_of
    return jnp.minimum(jnp.maximum(values, -limit), limit).astype(kind)


def setup_inputs(seed: int = 0) -> dict:
    seeds = jax.random.split(jax.random.key(seed), 13)
    items_table = gaussian(seeds[0], (ITEMS, D), 1.0, 6.0, ((0, 16),))
    fetch_rows = draw_fetch_rows(jax.random.fold_in(seeds[12], 71), 0)
    neighbour_slots = draw_neighbour_slots(jax.random.fold_in(seeds[12], 71), 0)
    neighbour_count = draw_neighbour_count(jax.random.fold_in(seeds[12], 71), 0)
    self_slot = place_ends(jax.random.randint(seeds[4], (NEG,), 0, N_NEG * CAP), jax.random.fold_in(seeds[4], 1), 0, (N_NEG * CAP) - 1).astype(jnp.int32)
    negative_count = place_ends(jax.random.randint(seeds[5], (NEG,), 1, 1000), jax.random.fold_in(seeds[5], 1), 1, 999).astype(jnp.int32)
    message_weight = gaussian(seeds[6], (D, D), D ** -0.5, 0.25)
    message_bias = gaussian(seeds[7], (D,), 0.5, 3.0, (), jnp.float32)
    self_weight = gaussian(seeds[8], (D, D), D ** -0.5, 0.25)
    neighbour_weight = gaussian(seeds[9], (D, D), D ** -0.5, 0.25)
    output_bias = gaussian(seeds[10], (D,), 0.5, 3.0, (), jnp.float32)
    queries = draw_queries(jax.random.fold_in(seeds[12], 71), 0)
    return {"items_table": items_table, "fetch_rows": fetch_rows, "neighbour_slots": neighbour_slots, "neighbour_count": neighbour_count, "self_slot": self_slot, "negative_count": negative_count, "message_weight": message_weight, "message_bias": message_bias, "self_weight": self_weight, "neighbour_weight": neighbour_weight, "output_bias": output_bias, "queries": queries}


def embed_device(items_table, fetch_block, slot_block, count_block, self_block, message_weight, message_bias, self_weight, neighbour_weight, output_bias):
    owners = jnp.arange(N_NEG, dtype=jnp.int32)[:, None] * ITEM_DEV
    global_rows = (fetch_block.astype(jnp.int32) + owners).reshape(-1)
    fetched = items_table[global_rows]
    message = jax.nn.relu(jnp.dot(fetched, message_weight, preferred_element_type=jnp.float32) + message_bias).astype(jnp.bfloat16)
    gathered = message[slot_block].astype(jnp.float32)
    live_mask = jnp.arange(K, dtype=jnp.int32)[None, :] < count_block[:, None]
    summed = lax.optimization_barrier(jnp.sum(jnp.where(live_mask[:, :, None], gathered, jnp.float32(0.0)), axis=1))
    neighbour_mean = (summed / count_block.astype(jnp.float32)[:, None]).astype(jnp.bfloat16)
    self_rows = fetched[self_block]
    hidden = jnp.dot(self_rows, self_weight, preferred_element_type=jnp.float32)
    hidden = hidden + jnp.dot(neighbour_mean, neighbour_weight, preferred_element_type=jnp.float32) + output_bias
    hidden = jax.nn.relu(hidden)
    scale_inv = lax.rsqrt(lax.optimization_barrier(jnp.mean(hidden * hidden, axis=-1, keepdims=True)) + 0.25)
    return (hidden * scale_inv).astype(jnp.bfloat16)

def reference(items_table, fetch_rows, neighbour_slots, neighbour_count, self_slot, negative_count, message_weight, message_bias, self_weight, neighbour_weight, output_bias, queries):
    devices_all = N_NEG * N_QRY
    fetch_all = fetch_rows.reshape(devices_all, N_NEG, -1)
    slots_all = neighbour_slots.reshape(devices_all, -1, K)
    counts_all = neighbour_count.reshape(devices_all, -1)
    selves_all = self_slot.reshape(devices_all, -1)

    def one_device(inputs):
        return embed_device(items_table, inputs[0], inputs[1], inputs[2], inputs[3], message_weight, message_bias, self_weight, neighbour_weight, output_bias)
    embedded = lax.map(one_device, (fetch_all, slots_all, counts_all, selves_all))
    negative_embed = embedded.reshape(-1, D)
    log_count = jnp.log(negative_count.astype(jnp.float32))
    query_blocks = queries.reshape(N_QRY, -1, D)

    def one_block(query_block):
        scores = 0.25 * jnp.dot(query_block, negative_embed.T, preferred_element_type=jnp.float32) - log_count[None, :]
        peak = lax.optimization_barrier(jnp.max(scores, axis=1))
        totals = lax.optimization_barrier(jnp.sum(jnp.exp(scores - peak[:, None]), axis=1))
        return peak + jnp.log(totals) - math.log(NEG)
    query_lse = lax.map(one_block, query_blocks).reshape(-1)
    return (negative_embed, query_lse)
```

```python
import functools
import math

import jax
import jax.numpy as jnp
from jax import lax
from jax.experimental import pallas as pl
from jax.experimental.pallas import tpu as pltpu
from jax.sharding import PartitionSpec as P


SIDE = 4
HOPS = (
    ((2, 2), (0, 1)),
    ((2, 1), (0, -1)),
    ((3, 2), (1, 1)),
    ((2, 3), (0, -1)),
    ((1, 2), (1, -1)),
    ((2, 0), (0, 1)),
    ((0, 2), (1, 1)),
    ((1, 1), (0, 1)),
    ((1, 3), (1, -1)),
    ((3, 1), (1, 1)),
    ((3, 3), (0, -1)),
    ((1, 0), (0, 1)),
    ((0, 3), (1, -1)),
    ((0, 1), (1, 1)),
    ((3, 0), (0, -1)),
    ((0, 0), None),
)
BLOCK_VMEM = 9 * 2**20
ROWS = 48


def compact_kernel(owner_ref, local_ref, out_ref, count_ref):
    neighbours, width = local_ref.shape
    parts = out_ref.shape[1]
    part = lax.broadcasted_iota(jnp.int32, (parts, 128), 0).astype(jnp.int16)
    one = jnp.ones((parts, 128), jnp.int16)
    zero = jnp.zeros((parts, 128), jnp.int16)
    for t in range(width // 128):
        lanes = slice(128 * t, 128 * t + 128)
        seen = zero
        found = [zero - one] * neighbours
        for k in range(neighbours):
            owner = jnp.broadcast_to(owner_ref[k : k + 1, lanes], (parts, 128)).astype(jnp.int16)
            local = jnp.broadcast_to(local_ref[k : k + 1, lanes], (parts, 128)).astype(jnp.int16)
            mine = owner == part
            rank = jnp.where(mine, seen, zero - one)
            for j in range(k + 1):
                found[j] = jnp.where(rank == jnp.int16(j), local, found[j])
            seen = seen + jnp.where(mine, one, zero)
        for j in range(neighbours):
            out_ref[j, :, lanes] = found[j]
        count_ref[:, lanes] = seen.astype(jnp.int32)


def compact(owner, local, parts):
    neighbours, width = owner.shape
    return pl.pallas_call(
        compact_kernel,
        out_shape=(
            jax.ShapeDtypeStruct((neighbours, parts, width), jnp.int16),
            jax.ShapeDtypeStruct((parts, width), jnp.int32),
        ),
        name="compact",
        compiler_params=pltpu.CompilerParams(vmem_limit_bytes=8 * 2**20),
    )(owner, local)


def table_kernel(rows_ref, mw_ref, mb_ref, nw_ref, sw_ref, u_ref, v_ref):
    rows = rows_ref[...]
    count = rows.shape[0]
    message = jnp.dot(rows, mw_ref[...], preferred_element_type=jnp.float32) + mb_ref[...]
    message = jnp.maximum(message, 0.0).astype(jnp.bfloat16)
    u = jnp.dot(message, nw_ref[...], preferred_element_type=jnp.float32)
    v = jnp.dot(rows, sw_ref[...], preferred_element_type=jnp.float32)
    for j in range(4):
        u_ref[pl.ds(j, count, stride=4), :] = u[:, 128 * j : 128 * j + 128]
        v_ref[pl.ds(j, count, stride=4), :] = v[:, 128 * j : 128 * j + 128]


def tables(items, message_weight, message_bias, neighbour_weight, self_weight):
    items_count, width = items.shape
    tile = 512
    whole = pl.BlockSpec((width, width), lambda i: (0, 0))
    out = pl.BlockSpec((4 * tile, 128), lambda i: (i, 0))
    shape = pltpu.VMEM((4 * items_count, 128), jnp.float32)
    return pl.pallas_call(
        table_kernel,
        grid=(items_count // tile,),
        in_specs=[
            pl.BlockSpec((tile, width), lambda i: (i, 0)),
            whole,
            pl.BlockSpec((1, width), lambda i: (0, 0)),
            whole,
            whole,
        ],
        out_specs=(out, out),
        out_shape=(shape, shape),
        name="tables",
        cost_estimate=pl.CostEstimate(
            flops=6 * items_count * width * width, bytes_accessed=40 * 2**20, transcendentals=0
        ),
        compiler_params=pltpu.CompilerParams(vmem_limit_bytes=12 * 2**20),
    )(items, message_weight, message_bias[None], neighbour_weight, self_weight)


def owner_kernel(arrivals, n_ref, fetch_ref, self_ref, most_ref, slots_ref, u_ref, v_ref, *refs):
    parts, (out_ref, g_ref, z_ref, a_ref) = refs[:arrivals], refs[-4:]
    cap = a_ref.shape[1]
    count, neighbours = slots_ref.shape[1], slots_ref.shape[2] - 2
    unroll = 16

    def fetch(t, _):
        for r in range(unroll):
            s = t * unroll + r
            row = fetch_ref[0, 0, s]
            g_ref[pl.ds(pl.multiple_of(s * 4, 4), 4), :] = u_ref[
                pl.ds(pl.multiple_of(row * 4, 4), 4), :
            ]
        return 0

    lax.fori_loop(0, cap // unroll, fetch, 0)

    def own(t, _):
        for r in range(unroll):
            v = t * unroll + r
            row = fetch_ref[0, 0, self_ref[0, 0, v]]
            z_ref[pl.ds(pl.multiple_of(v * 4, 4), 4), :] = v_ref[
                pl.ds(pl.multiple_of(row * 4, 4), 4), :
            ]
        return 0

    lax.fori_loop(0, count // unroll, own, 0)

    chunks = cap // 128
    tile = 16
    lane = lax.broadcasted_iota(jnp.int32, (tile, 128), 1)
    lanes = [(lane + 128 * c).astype(jnp.int16) for c in range(chunks)]
    one = jnp.ones((tile, 128), jnp.bfloat16)
    zero = jnp.zeros((tile, 128), jnp.bfloat16)

    def build(t, _):
        at = pl.ds(pl.multiple_of(t * tile, tile), tile)
        slots = slots_ref[0, at, :]
        most = most_ref[0, 0, t]

        def add(first, last, total):
            for k in range(first, last):
                slot = jnp.broadcast_to(slots[:, k : k + 1], (tile, 128))
                total = [
                    total[c] + jnp.where(slot == lanes[c], one, zero) for c in range(chunks)
                ]
            return total

        def put(total):
            for c in range(chunks):
                a_ref[at, 128 * c : 128 * c + 128] = total[c]

        put(add(0, 4, [zero] * chunks))

        def more(first, step):
            if first >= neighbours:
                return

            @pl.when(most > first)
            def _():
                last = min(first + step, neighbours)
                held = [a_ref[at, 128 * c : 128 * c + 128] for c in range(chunks)]
                put(add(first, last, held))
                more(last, step if last < 12 else 7)

        more(4, 2)
        return 0

    lax.fori_loop(0, count // tile, build, 0)

    gathered = jnp.concatenate(
        [g_ref[pl.ds(j, cap, stride=4), :].astype(jnp.bfloat16) for j in range(4)], axis=1
    )
    half = count // 2
    for h in range(2):
        at = slice(h * half, h * half + half)
        mean = jnp.dot(a_ref[at, :], gathered, preferred_element_type=jnp.float32)
        last = slots_ref[0, at, neighbours:].astype(jnp.int32).astype(jnp.float32)
        mask = last[:, 0:1] >= 0.0
        mean = mean * (1.0 / last[:, 1:2])
        for j in range(4):
            cols = slice(128 * j, 128 * j + 128)
            own = z_ref[pl.ds(h * half * 4 + j, half, stride=4), :]
            total = mean[:, cols] + jnp.where(mask, own, 0.0)
            for part in parts:
                total = total + part[at, cols].astype(jnp.float32)
            out_ref[at, cols] = total.astype(out_ref.dtype)


def owner_block(step, n, fetch, selves, most, slots, u, v, parts, before, kind):
    _, _, cap = fetch.shape
    _, count, rows = slots.shape

    def smem(width):
        return pl.BlockSpec((1, 1, width), lambda i, n: (n[step], 0, 0), memory_space=pltpu.SMEM)

    table = pl.BlockSpec(memory_space=pltpu.VMEM)
    anywhere = pl.BlockSpec(memory_space=pl.ANY)
    block = pl.BlockSpec((count, 512), lambda i, n: (0, 0))
    return pl.pallas_call(
        functools.partial(owner_kernel, len(parts)),
        grid_spec=pltpu.PrefetchScalarGridSpec(
            num_scalar_prefetch=1,
            grid=(1,),
            in_specs=[
                smem(cap), smem(count), smem(most.shape[2]),
                pl.BlockSpec((1, count, rows), lambda i, n: (n[step], 0, 0)),
                table, table, *[block] * len(parts), *[anywhere] * len(before),
            ],
            out_specs=block,
            scratch_shapes=[
                pltpu.VMEM((4 * cap, 128), jnp.float32),
                pltpu.VMEM((4 * count, 128), jnp.float32),
                pltpu.VMEM((count, cap), jnp.bfloat16),
            ],
        ),
        out_shape=jax.ShapeDtypeStruct((count, 512), kind),
        name="owner_block",
        cost_estimate=pl.CostEstimate(
            flops=3 * 10**9, bytes_accessed=4 * 2**20, transcendentals=0
        ),
        compiler_params=pltpu.CompilerParams(vmem_limit_bytes=BLOCK_VMEM),
    )(n, fetch, selves, most, slots, u, v, *parts, *before)


def score_kernel(negative_ref, log_ref, queries_ref, peak_ref, total_ref, column_ref):
    @pl.when(pl.program_id(0) == 0)
    def _():
        wide = jnp.broadcast_to(log_ref[...], (8, log_ref.shape[1]))
        column_ref[...] = jnp.transpose(wide)[:, 0:1]

    scores = lax.dot_general(
        negative_ref[...], queries_ref[...], (((1,), (1,)), ((), ())),
        preferred_element_type=jnp.float32,
    )
    scores = 0.25 * scores - column_ref[...]
    peak = jnp.max(scores, axis=0, keepdims=True)
    peak_ref[0] = peak
    total_ref[0] = jnp.sum(jnp.exp(scores - peak), axis=0, keepdims=True)


def score(negatives, log_count, queries):
    count, width = negatives.shape
    tile = 512
    tiles = queries.shape[0] // tile
    out = pl.BlockSpec((1, 1, tile), lambda i: (i, 0, 0))
    shape = jax.ShapeDtypeStruct((tiles, 1, tile), jnp.float32)
    peak, total = pl.pallas_call(
        score_kernel,
        grid=(tiles,),
        in_specs=[
            pl.BlockSpec((count, width), lambda i: (0, 0)),
            pl.BlockSpec((1, count), lambda i: (0, 0)),
            pl.BlockSpec((tile, width), lambda i: (i, 0)),
        ],
        out_specs=(out, out),
        out_shape=(shape, shape),
        scratch_shapes=[pltpu.VMEM((count, 1), jnp.float32)],
        name="score",
        cost_estimate=pl.CostEstimate(
            flops=2 * count * width * queries.shape[0], bytes_accessed=9 * 2**20, transcendentals=0
        ),
        compiler_params=pltpu.CompilerParams(vmem_limit_bytes=16 * 2**20),
    )(negatives, log_count, queries)
    return peak.reshape(-1), total.reshape(-1)


def shift(x, axis, step):
    pairs = []
    for a in range(SIDE):
        for b in range(SIDE):
            to = ((a + step) % SIDE, b) if axis == 0 else (a, (b + step) % SIDE)
            pairs.append((a * SIDE + b, to[0] * SIDE + to[1]))
    return lax.ppermute(x, "neg", pairs)


def joined(parts):
    peak = jnp.max(parts[:, 0], axis=0)
    total = jnp.sum(parts[:, 1] * jnp.exp(parts[:, 0] - peak[None]), axis=0)
    return jnp.stack([peak, total])


def per_device(
    items_table,
    fetch_rows,
    neighbour_slots,
    neighbour_count,
    self_slot,
    negative_count,
    message_weight,
    message_bias,
    self_weight,
    neighbour_weight,
    output_bias,
    queries,
):
    parts, cap = fetch_rows.shape
    count, neighbours = neighbour_slots.shape
    queries_all = lax.all_gather(queries, "qry", axis=0, tiled=True)

    slots = neighbour_slots.T
    live = jnp.arange(neighbours, dtype=jnp.int32)[:, None] < neighbour_count[None, :]
    owner = slots // cap
    local = slots - owner * cap
    found, counts = compact(jnp.where(live, owner, -1), local, parts)
    most = jnp.max(counts.reshape(parts, count // 16, 16), axis=2)
    self_local = self_slot[None, :] - (jnp.arange(parts, dtype=jnp.int32) * cap)[:, None]
    self_local = jnp.where((self_local >= 0) & (self_local < cap), self_local, -1)
    rest = jnp.concatenate(
        [
            self_local,
            jnp.broadcast_to(neighbour_count[None, :], (parts, count)),
            jnp.pad(most, ((0, 0), (0, count - most.shape[1]))),
            jnp.pad(fetch_rows, ((0, 0), (0, (ROWS - neighbours - 3) * count - cap))),
        ],
        axis=1,
    ).astype(jnp.int16)
    slab = jnp.concatenate(
        [found.transpose(1, 0, 2), rest.reshape(parts, ROWS - neighbours, count)], axis=1
    )
    slab = lax.all_to_all(slab, "neg", split_axis=0, concat_axis=0, tiled=True)

    slots_in = slab[:, : neighbours + 2].transpose(0, 2, 1)
    rest = slab[:, neighbours:].astype(jnp.int32)
    self_in = jnp.maximum(rest[:, 0], 0)[:, None, :]
    most_in = rest[:, 2, : count // 16][:, None, :]
    fetch_in = rest[:, 3:].reshape(parts, -1)[:, :cap][:, None, :]

    here = lax.axis_index("neg")
    x, y = here // SIDE, here % SIDE
    ns = [((x + dx) % SIDE) * SIDE + (y + dy) % SIDE for (dx, dy), _ in HOPS]
    qry = lax.axis_index("qry")
    own_count = lax.dynamic_slice_in_dim(negative_count, qry * count, count)
    log_count = jnp.log(own_count.astype(jnp.float32))[None, :]

    held = pltpu.with_memory_space_constraint(items_table, pltpu.HBM)
    held, slots_in, self_in, most_in, fetch_in, ns, log_count = lax.optimization_barrier(
        (held, slots_in, self_in, most_in, fetch_in, jnp.stack(ns), log_count)
    )
    u, v = tables(held, message_weight, message_bias, neighbour_weight, self_weight)

    arrived = {}
    before = []
    for k, ((dx, dy), way) in enumerate(HOPS):
        block = owner_block(
            k, ns, fetch_in, self_in, most_in, slots_in, u, v,
            arrived.get((dx, dy), []), before,
            jnp.float32 if way is None else jnp.bfloat16,
        )
        before = [block]
        if way is not None:
            axis, step = way
            to = ((dx - step) % SIDE, dy) if axis == 0 else (dx, (dy - step) % SIDE)
            arrived.setdefault(to, []).append(shift(block, axis, step))
    hidden = block

    hidden = jax.nn.relu(hidden + output_bias)
    scale_inv = lax.rsqrt(jnp.mean(hidden * hidden, axis=-1, keepdims=True) + 0.25)
    negative_embed = (hidden * scale_inv).astype(jnp.bfloat16)

    peak, total = score(negative_embed, log_count, queries_all)

    qrys = lax.axis_size("qry")
    pieces = jnp.stack([peak.reshape(qrys, -1), total.reshape(qrys, -1)], axis=1)
    pieces = lax.all_to_all(pieces, "qry", split_axis=0, concat_axis=0, tiled=True)
    pieces = lax.all_gather(joined(pieces), "neg", axis=0, tiled=False)
    peak, total = joined(pieces)
    negatives_all = count * lax.axis_size("neg") * qrys
    query_lse = peak + jnp.log(total) - math.log(negatives_all)
    return (negative_embed, query_lse)


def solution(mesh):
    in_specs = (
        P("neg", None),
        P(("neg", "qry"), None),
        P(("neg", "qry"), None),
        P(("neg", "qry")),
        P(("neg", "qry")),
        P("neg"),
        P(),
        P(),
        P(),
        P(),
        P(),
        P("qry", None),
    )
    out_specs = (P(("neg", "qry"), None), P("qry"))
    return jax.shard_map(
        per_device, mesh=mesh, in_specs=in_specs, out_specs=out_specs, check_vma=False
    )
```

```python
import functools
import math

import jax
import jax.numpy as jnp
from jax import lax
from jax.experimental import pallas as pl
from jax.experimental.pallas import tpu as pltpu
from jax.sharding import PartitionSpec as P


SIDE = 4
HOPS = (
    ((2, 2), (0, 1)),
    ((2, 1), (0, -1)),
    ((3, 2), (1, 1)),
    ((2, 3), (0, -1)),
    ((2, 0), (0, 1)),
    ((0, 2), (1, 1)),
    ((1, 1), (0, 1)),
    ((1, 2), (1, -1)),
    ((3, 1), (1, 1)),
    ((1, 3), (1, -1)),
    ((3, 3), (0, -1)),
    ((0, 3), (1, -1)),
    ((1, 0), (0, 1)),
    ((0, 1), (1, 1)),
    ((3, 0), (0, -1)),
    ((0, 0), None),
)
PLACE = {offset: k for k, (offset, _) in enumerate(HOPS)}
CHILDREN = [[] for _ in HOPS]
for _k, ((_dx, _dy), _way) in enumerate(HOPS):
    if _way is not None:
        _to = ((_dx - _way[1]) % SIDE, _dy) if _way[0] == 0 else (_dx, (_dy - _way[1]) % SIDE)
        CHILDREN[PLACE[_to]].append(_k)
LEAVES = [k for k in range(len(HOPS)) if not CHILDREN[k]]
INNER = [k for k in range(len(HOPS)) if CHILDREN[k]]
ORDER = (
    ((1, 2), 0), ((1, 2), 1), ((3, 1), 0), ((3, 1), 1), ((1, 3), 0), ((3, 3), 0), ((1, 3), 1),
    ((0, 3), 0), "near", ((3, 3), 1), ((1, 0), 0), ((1, 0), 1), ((0, 3), 1), ((0, 1), 0),
    ((3, 0), 0), ((0, 1), 1), ((3, 0), 1), "far",
)
ROWS = 48


def compact_kernel(owner_ref, local_ref, out_ref, count_ref):
    neighbours, width = local_ref.shape
    parts = out_ref.shape[1]
    part = lax.broadcasted_iota(jnp.int32, (parts, 128), 0).astype(jnp.int16)
    one = jnp.ones((parts, 128), jnp.int16)
    zero = jnp.zeros((parts, 128), jnp.int16)
    for t in range(width // 128):
        lanes = slice(128 * t, 128 * t + 128)
        seen = zero
        found = [zero - one] * neighbours
        for k in range(neighbours):
            owner = jnp.broadcast_to(owner_ref[k : k + 1, lanes], (parts, 128)).astype(jnp.int16)
            local = jnp.broadcast_to(local_ref[k : k + 1, lanes], (parts, 128)).astype(jnp.int16)
            mine = owner == part
            rank = jnp.where(mine, seen, zero - one)
            for j in range(k + 1):
                found[j] = jnp.where(rank == jnp.int16(j), local, found[j])
            seen = seen + jnp.where(mine, one, zero)
        for j in range(neighbours):
            out_ref[j, :, lanes] = found[j]
        count_ref[:, lanes] = seen.astype(jnp.int32)


def compact(owner, local, parts):
    neighbours, width = owner.shape
    return pl.pallas_call(
        compact_kernel,
        out_shape=(
            jax.ShapeDtypeStruct((neighbours, parts, width), jnp.int16),
            jax.ShapeDtypeStruct((parts, width), jnp.int32),
        ),
        name="compact",
        compiler_params=pltpu.CompilerParams(vmem_limit_bytes=8 * 2**20),
    )(owner, local)


def table_kernel(rows_ref, mw_ref, mb_ref, nw_ref, sw_ref, u_ref, v_ref):
    rows = rows_ref[...]
    count = rows.shape[0]
    message = jnp.dot(rows, mw_ref[...], preferred_element_type=jnp.float32) + mb_ref[...]
    message = jnp.maximum(message, 0.0).astype(jnp.bfloat16)
    u = jnp.dot(message, nw_ref[...], preferred_element_type=jnp.float32)
    v = jnp.dot(rows, sw_ref[...], preferred_element_type=jnp.float32)
    for j in range(4):
        u_ref[pl.ds(j, count, stride=4), :] = u[:, 128 * j : 128 * j + 128]
        v_ref[pl.ds(j, count, stride=4), :] = v[:, 128 * j : 128 * j + 128]


def tables(items, message_weight, message_bias, neighbour_weight, self_weight):
    items_count, width = items.shape
    tile = 512
    whole = pl.BlockSpec((width, width), lambda i: (0, 0))
    out = pl.BlockSpec((4 * tile, 128), lambda i: (i, 0))
    shape = pltpu.VMEM((4 * items_count, 128), jnp.float32)
    return pl.pallas_call(
        table_kernel,
        grid=(items_count // tile,),
        in_specs=[
            pl.BlockSpec((tile, width), lambda i: (i, 0)),
            whole,
            pl.BlockSpec((1, width), lambda i: (0, 0)),
            whole,
            whole,
        ],
        out_specs=(out, out),
        out_shape=(shape, shape),
        name="tables",
        cost_estimate=pl.CostEstimate(
            flops=6 * items_count * width * width, bytes_accessed=40 * 2**20, transcendentals=0
        ),
        compiler_params=pltpu.CompilerParams(vmem_limit_bytes=8 * 2**20),
    )(items, message_weight, message_bias[None], neighbour_weight, self_weight)


def owner_kernel(
    n_ref, fetch_ref, self_ref, most_ref, slots_ref, u_ref, v_ref, out_ref, g_ref, z_ref, a_ref
):
    cap = a_ref.shape[1]
    count, neighbours = slots_ref.shape[1], slots_ref.shape[2] - 2
    unroll = 16

    def fetch(t, _):
        for r in range(unroll):
            s = t * unroll + r
            row = fetch_ref[0, 0, s]
            g_ref[pl.ds(pl.multiple_of(s * 4, 4), 4), :] = u_ref[
                pl.ds(pl.multiple_of(row * 4, 4), 4), :
            ]
        return 0

    lax.fori_loop(0, cap // unroll, fetch, 0)

    def own(t, _):
        for r in range(unroll):
            v = t * unroll + r
            row = fetch_ref[0, 0, self_ref[0, 0, v]]
            z_ref[pl.ds(pl.multiple_of(v * 4, 4), 4), :] = v_ref[
                pl.ds(pl.multiple_of(row * 4, 4), 4), :
            ]
        return 0

    lax.fori_loop(0, count // unroll, own, 0)

    chunks = cap // 128
    tile = 16
    pair = 2
    lane = lax.broadcasted_iota(jnp.int32, (tile, 128), 1)
    lanes = [(lane + 128 * c).astype(jnp.int16) for c in range(chunks)]
    one = jnp.ones((tile, 128), jnp.bfloat16)
    zero = jnp.zeros((tile, 128), jnp.bfloat16)

    def build(t, _):
        ats = [pl.ds(pl.multiple_of((t * pair + i) * tile, tile), tile) for i in range(pair)]
        slots = [slots_ref[0, at, :] for at in ats]
        most = most_ref[0, 0, t]

        def add(first, last, totals):
            for k in range(first, last):
                for i in range(pair):
                    slot = jnp.broadcast_to(slots[i][:, k : k + 1], (tile, 128))
                    totals[i] = [
                        totals[i][c] + jnp.where(slot == lanes[c], one, zero)
                        for c in range(chunks)
                    ]
            return totals

        def put(totals):
            for i in range(pair):
                for c in range(chunks):
                    a_ref[ats[i], 128 * c : 128 * c + 128] = totals[i][c]

        put(add(0, 6, [[zero] * chunks for _ in range(pair)]))

        def more(first, step):
            if first >= neighbours:
                return

            @pl.when(most > first)
            def _():
                last = min(first + step, neighbours)
                held = [
                    [a_ref[ats[i], 128 * c : 128 * c + 128] for c in range(chunks)]
                    for i in range(pair)
                ]
                put(add(first, last, held))
                more(last, 2 * step)

        more(6, 2)
        return 0

    lax.fori_loop(0, count // (tile * pair), build, 0)

    gathered = jnp.concatenate(
        [g_ref[pl.ds(j, cap, stride=4), :].astype(jnp.bfloat16) for j in range(4)], axis=1
    )
    half = count // 2
    for h in range(2):
        at = slice(h * half, h * half + half)
        mean = jnp.dot(a_ref[at, :], gathered, preferred_element_type=jnp.float32)
        last = slots_ref[0, at, neighbours:].astype(jnp.int32).astype(jnp.float32)
        mask = last[:, 0:1] >= 0.0
        mean = mean * (1.0 / last[:, 1:2])
        for j in range(4):
            cols = slice(128 * j, 128 * j + 128)
            own = z_ref[pl.ds(h * half * 4 + j, half, stride=4), :]
            total = mean[:, cols] + jnp.where(mask, own, 0.0)
            out_ref[0, at, cols] = total.astype(out_ref.dtype)


def owner_blocks(n, fetch, selves, most, slots, u, v):
    parts, _, cap = fetch.shape
    _, count, rows = slots.shape

    def smem(width):
        return pl.BlockSpec((1, 1, width), lambda i, n: (n[i], 0, 0), memory_space=pltpu.SMEM)

    table = pl.BlockSpec(memory_space=pltpu.VMEM)
    return pl.pallas_call(
        owner_kernel,
        grid_spec=pltpu.PrefetchScalarGridSpec(
            num_scalar_prefetch=1,
            grid=(parts,),
            in_specs=[
                smem(cap), smem(count), smem(most.shape[2]),
                pl.BlockSpec((1, count, rows), lambda i, n: (n[i], 0, 0)),
                table, table,
            ],
            out_specs=pl.BlockSpec((1, count, 512), lambda i, n: (i, 0, 0)),
            scratch_shapes=[
                pltpu.VMEM((4 * cap, 128), jnp.float32),
                pltpu.VMEM((4 * count, 128), jnp.float32),
                pltpu.VMEM((count, cap), jnp.bfloat16),
            ],
        ),
        out_shape=pltpu.HBM((parts, count, 512), jnp.bfloat16),
        name="owner_blocks",
        cost_estimate=pl.CostEstimate(
            flops=45 * 10**9, bytes_accessed=44 * 2**20, transcendentals=0
        ),
        compiler_params=pltpu.CompilerParams(vmem_limit_bytes=9 * 2**20),
    )(n, fetch, selves, most, slots, u, v)


MESH = pl.DeviceIdType.MESH


def join(peak, total, other_peak, other_total):
    top = jnp.maximum(peak, other_peak)
    return top, total * jnp.exp(peak - top) + other_total * jnp.exp(other_peak - top)


def tower_kernel(
    parts, qrys, blocks_ref, bias_ref, log_ref, queries_ref, negative_ref, lse_ref,
    landed, summed, gathered, column_ref, partial, first_in, second_out, second_in,
    load_sem, block_send, block_recv, query_send, query_recv, own_sem, first_send, first_recv, second_send,
    second_recv,
):
    n, q = lax.axis_index("neg"), lax.axis_index("qry")
    x, y = n // SIDE, n % SIDE
    z, core = q // 2, q % 2
    count = blocks_ref.shape[1]
    own_rows = queries_ref.shape[0]
    half = count // 2

    barrier = pltpu.get_barrier_semaphore()
    for i in range(1, qrys):
        pl.semaphore_signal(
            barrier, inc=1, device_id=(n, lax.rem(q + i, qrys)), device_id_type=MESH
        )
    for i in range(1, parts):
        pl.semaphore_signal(
            barrier, inc=1, device_id=(lax.rem(n + i, parts), q), device_id_type=MESH
        )
    pl.semaphore_wait(barrier, qrys + parts - 2)

    def hop(k, h):
        axis, step = HOPS[k][1]
        if axis == 0:
            to = lax.rem(x + step + SIDE, SIDE) * SIDE + y
        else:
            to = x * SIDE + lax.rem(y + step + SIDE, SIDE)
        rows = pl.ds(h * half, half)
        source = summed.at[INNER.index(k), rows] if k in INNER else blocks_ref.at[k, rows]
        return pltpu.make_async_remote_copy(
            src_ref=source, dst_ref=landed.at[k, rows],
            send_sem=block_send.at[k, h], recv_sem=block_recv.at[k, h],
            device_id=(to, q), device_id_type=MESH,
        )

    up = (n, lax.rem(z + 1, qrys // 2) * 2 + core)
    down = (n, lax.rem(z + qrys // 2 - 1, qrys // 2) * 2 + core)
    partner = (n, z * 2 + 1 - core)
    below, above = down[1], up[1]
    across = lax.rem(z + 2, qrys // 2) * 2 + core

    def spread(k, block, part, to, source=None):
        rows = pl.ds(0, own_rows) if part is None else pl.ds(part * (own_rows // 2), own_rows // 2)
        return pltpu.make_async_remote_copy(
            src_ref=gathered.at[block, rows] if source is None else source,
            dst_ref=gathered.at[block, rows],
            send_sem=query_send.at[k], recv_sem=query_recv.at[k],
            device_id=to, device_id_type=MESH,
        )

    spreads = [
        spread(0, q, None, up, queries_ref),
        spread(1, q, None, down, queries_ref),
        spread(2, q, None, partner, queries_ref),
        spread(3, below, 0, up),
        spread(4, above, 1, down),
        spread(5, below, None, partner),
        spread(6, above, None, partner),
        spread(7, across, 0, partner),
        spread(8, across, 1, partner),
    ]

    hops = {(k, h): hop(k, h) for k in range(len(HOPS) - 1) for h in range(2)}
    for k in LEAVES[:3]:
        for h in range(2):
            hops[k, h].start()
    for k in range(3):
        spreads[k].start()
    for k in LEAVES[3:]:
        for h in range(2):
            hops[k, h].start()
    loads = {}
    for i, k in enumerate(INNER):
        loads[k] = pltpu.make_async_copy(blocks_ref.at[k], summed.at[i], load_sem.at[i])
        loads[k].start()
    own = pltpu.make_async_copy(queries_ref, gathered.at[q], own_sem)
    own.start()
    wide = jnp.broadcast_to(log_ref[...], (8, count))
    column_ref[...] = jnp.transpose(wide)[:, 0:1]

    step = 64

    def form(k, h):
        if h == 0:
            loads[k].wait()
        for child in CHILDREN[k]:
            hops[child, h].wait_recv()

        def body(t, _):
            rows = pl.ds(pl.multiple_of(h * half + t * step, step), step)
            total = summed[INNER.index(k), rows, :].astype(jnp.float32)
            for child in CHILDREN[k]:
                total = total + landed[child, rows, :].astype(jnp.float32)
            if HOPS[k][1] is None:
                hidden = jnp.maximum(total + bias_ref[...], 0.0)
                mean = jnp.mean(hidden * hidden, axis=-1, keepdims=True)
                negative_ref[rows, :] = (hidden * lax.rsqrt(mean + 0.25)).astype(jnp.bfloat16)
            else:
                summed[INNER.index(k), rows, :] = total.astype(jnp.bfloat16)
            return 0

        lax.fori_loop(0, half // step, body, 0)

    for entry in ORDER:
        if entry == "near":
            spreads[0].wait_recv()
            spreads[3].start()
            spreads[5].start()
            spreads[1].wait_recv()
            spreads[4].start()
            spreads[6].start()
        elif entry == "far":
            spreads[3].wait_recv()
            spreads[7].start()
            spreads[4].wait_recv()
            spreads[8].start()
        else:
            k = PLACE[entry[0]]
            form(k, entry[1])
            hops[k, entry[1]].start()
    root = len(HOPS) - 1
    for h in range(2):
        form(root, h)
    own.wait()
    for k in (2, 5, 6, 7, 8):
        spreads[k].wait_recv()

    tile = 512

    def score(block):
        for t in range(own_rows // tile):
            cols = slice(t * tile, t * tile + tile)
            scores = lax.dot_general(
                negative_ref[...], gathered[block, cols, :], (((1,), (1,)), ((), ())),
                preferred_element_type=jnp.float32,
            )
            scores = 0.25 * scores - column_ref[...]
            peak = jnp.max(scores, axis=0, keepdims=True)
            partial[block, 0:1, cols] = peak
            partial[block, 1:2, cols] = jnp.sum(jnp.exp(scores - peak), axis=0, keepdims=True)

    def first(i):
        to = lax.rem(q + i, qrys)
        return pltpu.make_async_remote_copy(
            src_ref=partial.at[to], dst_ref=first_in.at[i],
            send_sem=first_send.at[i], recv_sem=first_recv.at[i],
            device_id=(n, to), device_id_type=MESH,
        )

    def each(i, _):
        score(lax.rem(q + i, qrys))

        @pl.when(i > 1)
        def _():
            first(i - 1).start()

        return 0

    lax.fori_loop(1, qrys, each, 0)
    score(q)
    first(qrys - 1).start()
    peak, total = partial[q, 0:1, :], partial[q, 1:2, :]
    for i in range(1, qrys):
        first(i).wait_recv()
        peak, total = join(peak, total, first_in[i, 0:1, :], first_in[i, 1:2, :])
    second_out[0:1, :] = peak
    second_out[1:2, :] = total

    def second(i):
        return pltpu.make_async_remote_copy(
            src_ref=second_out, dst_ref=second_in.at[i],
            send_sem=second_send.at[i], recv_sem=second_recv.at[i],
            device_id=(lax.rem(n + i, parts), q), device_id_type=MESH,
        )

    for i in range(1, parts):
        second(i).start()
    for k in range(len(HOPS) - 1):
        for h in range(2):
            hops[k, h].wait_send()
    for k in range(9):
        spreads[k].wait_send()
    for i in range(1, qrys):
        first(i).wait_send()
    for i in range(1, parts):
        second(i).wait_recv()
        peak, total = join(peak, total, second_in[i, 0:1, :], second_in[i, 1:2, :])
    lse_ref[...] = peak + jnp.log(total) - math.log(count * parts * qrys)
    for i in range(1, parts):
        second(i).wait_send()


def tower(blocks, bias, log_count, queries, qrys):
    parts, count, width = blocks.shape
    own_rows = queries.shape[0]
    vmem = pl.BlockSpec(memory_space=pltpu.VMEM)
    dma = pltpu.SemaphoreType.DMA
    hops = len(HOPS) - 1
    return pl.pallas_call(
        functools.partial(tower_kernel, parts, qrys),
        in_specs=[pl.BlockSpec(memory_space=pltpu.HBM), vmem, vmem, vmem],
        out_specs=(vmem, vmem),
        out_shape=(
            jax.ShapeDtypeStruct((count, width), jnp.bfloat16),
            jax.ShapeDtypeStruct((1, own_rows), jnp.float32),
        ),
        scratch_shapes=[
            pltpu.VMEM((hops, count, width), jnp.bfloat16),
            pltpu.VMEM((len(INNER), count, width), jnp.bfloat16),
            pltpu.VMEM((qrys, own_rows, width), jnp.bfloat16),
            pltpu.VMEM((count, 1), jnp.float32),
            pltpu.VMEM((qrys, 2, own_rows), jnp.float32),
            pltpu.VMEM((qrys, 2, own_rows), jnp.float32),
            pltpu.VMEM((2, own_rows), jnp.float32),
            pltpu.VMEM((parts, 2, own_rows), jnp.float32),
            dma((len(INNER),)), dma((hops, 2)), dma((hops, 2)), dma((9,)), dma((9,)), dma,
            dma((qrys,)), dma((qrys,)), dma((parts,)), dma((parts,)),
        ],
        name="tower",
        compiler_params=pltpu.CompilerParams(
            collective_id=0, has_side_effects=True, vmem_limit_bytes=40 * 2**20
        ),
    )(blocks, bias, log_count, queries)


def per_device(
    items_table,
    fetch_rows,
    neighbour_slots,
    neighbour_count,
    self_slot,
    negative_count,
    message_weight,
    message_bias,
    self_weight,
    neighbour_weight,
    output_bias,
    queries,
):
    parts, cap = fetch_rows.shape
    count, neighbours = neighbour_slots.shape

    slots = neighbour_slots.T
    live = jnp.arange(neighbours, dtype=jnp.int32)[:, None] < neighbour_count[None, :]
    owner = slots // cap
    local = slots - owner * cap
    found, counts = compact(jnp.where(live, owner, -1), local, parts)
    most = jnp.max(counts.reshape(parts, count // 32, 32), axis=2)
    self_local = self_slot[None, :] - (jnp.arange(parts, dtype=jnp.int32) * cap)[:, None]
    self_local = jnp.where((self_local >= 0) & (self_local < cap), self_local, -1)
    rest = jnp.concatenate(
        [
            self_local,
            jnp.broadcast_to(neighbour_count[None, :], (parts, count)),
            jnp.pad(most, ((0, 0), (0, count - most.shape[1]))),
            jnp.pad(fetch_rows, ((0, 0), (0, (ROWS - neighbours - 3) * count - cap))),
        ],
        axis=1,
    ).astype(jnp.int16)
    slab = jnp.concatenate(
        [found.transpose(1, 0, 2), rest.reshape(parts, ROWS - neighbours, count)], axis=1
    )
    slab = lax.all_to_all(slab, "neg", split_axis=0, concat_axis=0, tiled=True)

    slots_in = slab[:, : neighbours + 2].transpose(0, 2, 1)
    rest = slab[:, neighbours:].astype(jnp.int32)
    self_in = jnp.maximum(rest[:, 0], 0)[:, None, :]
    most_in = rest[:, 2, : count // 32][:, None, :]
    fetch_in = rest[:, 3:].reshape(parts, -1)[:, :cap][:, None, :]

    here = lax.axis_index("neg")
    x, y = here // SIDE, here % SIDE
    ns = [((x + dx) % SIDE) * SIDE + (y + dy) % SIDE for (dx, dy), _ in HOPS]
    qry = lax.axis_index("qry")
    own_count = lax.dynamic_slice_in_dim(negative_count, qry * count, count)
    log_count = jnp.log(own_count.astype(jnp.float32))[None, :]

    held = pltpu.with_memory_space_constraint(items_table, pltpu.HBM)
    held, slots_in, self_in, most_in, fetch_in, ns, log_count = lax.optimization_barrier(
        (held, slots_in, self_in, most_in, fetch_in, jnp.stack(ns), log_count)
    )
    u, v = tables(held, message_weight, message_bias, neighbour_weight, self_weight)

    blocks = owner_blocks(ns, fetch_in, self_in, most_in, slots_in, u, v)
    blocks = pltpu.with_memory_space_constraint(blocks, pltpu.HBM)
    negative_embed, query_lse = tower(
        blocks, output_bias[None], log_count, queries, lax.axis_size("qry")
    )
    return (negative_embed, query_lse[0])


def solution(mesh):
    in_specs = (
        P("neg", None),
        P(("neg", "qry"), None),
        P(("neg", "qry"), None),
        P(("neg", "qry")),
        P(("neg", "qry")),
        P("neg"),
        P(),
        P(),
        P(),
        P(),
        P(),
        P("qry", None),
    )
    out_specs = (P(("neg", "qry"), None), P("qry"))
    return jax.shard_map(
        per_device, mesh=mesh, in_specs=in_specs, out_specs=out_specs, check_vma=False
    )
```

```python
import functools
import math

import jax
import jax.numpy as jnp
from jax import lax
from jax.experimental import pallas as pl
from jax.experimental.pallas import tpu as pltpu
from jax.sharding import PartitionSpec as P


SIDE = 4
HOPS = (
    ((2, 2), (0, 1)),
    ((2, 1), (0, -1)),
    ((3, 2), (1, 1)),
    ((2, 0), (0, 1)),
    ((1, 2), (1, -1)),
    ((2, 3), (0, -1)),
    ((0, 2), (1, 1)),
    ((1, 1), (0, 1)),
    ((3, 1), (1, 1)),
    ((1, 3), (1, -1)),
    ((3, 3), (0, -1)),
    ((1, 0), (0, 1)),
    ((0, 1), (1, 1)),
    ((0, 3), (1, -1)),
    ((3, 0), (0, -1)),
    ((0, 0), None),
)
PLACE = {offset: k for k, (offset, _) in enumerate(HOPS)}
CHILDREN = [[] for _ in HOPS]
for _k, ((_dx, _dy), _way) in enumerate(HOPS):
    if _way is not None:
        _to = ((_dx - _way[1]) % SIDE, _dy) if _way[0] == 0 else (_dx, (_dy - _way[1]) % SIDE)
        CHILDREN[PLACE[_to]].append(_k)
NEAR, FAR = 4, 10
TOWER_VMEM = 62 * 2**20
ROWS = 48


def compact_kernel(owner_ref, local_ref, out_ref, count_ref):
    neighbours, width = local_ref.shape
    parts = out_ref.shape[1]
    part = lax.broadcasted_iota(jnp.int32, (parts, 128), 0).astype(jnp.int16)
    one = jnp.ones((parts, 128), jnp.int16)
    zero = jnp.zeros((parts, 128), jnp.int16)
    for t in range(width // 128):
        lanes = slice(128 * t, 128 * t + 128)
        seen = zero
        found = [zero - one] * neighbours
        for k in range(neighbours):
            owner = jnp.broadcast_to(owner_ref[k : k + 1, lanes], (parts, 128)).astype(jnp.int16)
            local = jnp.broadcast_to(local_ref[k : k + 1, lanes], (parts, 128)).astype(jnp.int16)
            mine = owner == part
            rank = jnp.where(mine, seen, zero - one)
            for j in range(k + 1):
                found[j] = jnp.where(rank == jnp.int16(j), local, found[j])
            seen = seen + jnp.where(mine, one, zero)
        for j in range(neighbours):
            out_ref[j, :, lanes] = found[j]
        count_ref[:, lanes] = seen.astype(jnp.int32)


def compact(owner, local, parts):
    neighbours, width = owner.shape
    return pl.pallas_call(
        compact_kernel,
        out_shape=(
            jax.ShapeDtypeStruct((neighbours, parts, width), jnp.int16),
            jax.ShapeDtypeStruct((parts, width), jnp.int32),
        ),
        name="compact",
        compiler_params=pltpu.CompilerParams(vmem_limit_bytes=8 * 2**20),
    )(owner, local)


def counts_kernel(n_ref, most_ref, slab_ref, out_ref):
    cap, count = out_ref.shape[1:]
    neighbours = slab_ref.shape[1] - 8
    tile = 16
    row = lax.broadcasted_iota(jnp.int32, (tile, 128), 0).astype(jnp.int16)
    zero = jnp.zeros((tile, 128), jnp.bfloat16)

    def build(t, _):
        lanes = pl.ds(pl.multiple_of(t * 128, 128), 128)
        rows = slab_ref[0, :, lanes].astype(jnp.int32)
        most = most_ref[0, 0, t]
        scale = 1.0 / rows[neighbours + 1 : neighbours + 2].astype(jnp.float32)
        scale = jnp.broadcast_to(scale, (tile, 128)).astype(jnp.bfloat16)

        def spread(k):
            return jnp.broadcast_to(rows[k : k + 1], (tile, 128)).astype(jnp.int16)

        slots = [spread(k) for k in range(6)]
        for i in range(cap // tile):
            here = row + jnp.int16(i * tile)
            total = jnp.where(slots[0] == here, scale, zero)
            for slot in slots[1:]:
                total = total + jnp.where(slot == here, scale, zero)
            out_ref[0, i * tile : (i + 1) * tile, lanes] = total

        def more(first, step):
            if first >= neighbours:
                return

            @pl.when(most > first)
            def _():
                last = min(first + step, neighbours)
                slots = [spread(k) for k in range(first, last)]

                def body(i, _):
                    at = pl.ds(pl.multiple_of(i * tile, tile), tile)
                    here = row + (i * tile).astype(jnp.int16)
                    total = out_ref[0, at, lanes]
                    for slot in slots:
                        total = total + jnp.where(slot == here, scale, zero)
                    out_ref[0, at, lanes] = total
                    return 0

                lax.fori_loop(0, cap // tile, body, 0, unroll=first < 8)
                more(last, 2 * step)

        more(6, 2)
        return 0

    lax.fori_loop(0, count // 128, build, 0)


def counts_blocks(n, most, slab, cap):
    parts, rows, count = slab.shape
    return pl.pallas_call(
        counts_kernel,
        grid_spec=pltpu.PrefetchScalarGridSpec(
            num_scalar_prefetch=1,
            grid=(parts,),
            in_specs=[
                pl.BlockSpec(
                    (1, 1, most.shape[2]), lambda i, n: (n[i], 0, 0), memory_space=pltpu.SMEM
                ),
                pl.BlockSpec((1, rows, count), lambda i, n: (n[i], 0, 0)),
            ],
            out_specs=pl.BlockSpec((1, cap, count), lambda i, n: (i, 0, 0)),
        ),
        out_shape=pltpu.HBM((parts, cap, count), jnp.bfloat16),
        name="counts",
        cost_estimate=pl.CostEstimate(
            flops=10**9, bytes_accessed=12 * 2**20, transcendentals=0
        ),
        compiler_params=pltpu.CompilerParams(vmem_limit_bytes=6 * 2**20),
    )(n, most, slab)


MESH = pl.DeviceIdType.MESH


def join(peak, total, other_peak, other_total):
    top = jnp.maximum(peak, other_peak)
    return top, total * jnp.exp(peak - top) + other_total * jnp.exp(other_peak - top)


def tower_kernel(
    parts, qrys, fetch_ref, self_ref, counts_ref, items_ref, mw_ref, mb_ref, nw_ref,
    sw_ref, bias_ref, log_ref, queries_ref, negative_ref, lse_ref, gathered,
    u_ref, v_ref, items_tile, landed, summed, matrix, g_ref, z_ref, column_ref, partial, first_in,
    second_out, second_in, items_sem, matrix_sem, tile_sem, block_send, block_recv, query_send,
    query_recv, first_send, first_recv, second_send, second_recv,
):
    n, q = lax.axis_index("neg"), lax.axis_index("qry")
    x, y = n // SIDE, n % SIDE
    z, core = q // 2, q % 2
    cap, count = counts_ref.shape[1:]
    own_rows = queries_ref.shape[0]
    half = count // 2

    def matrix_load(k):
        slot = lax.rem(k, 2)
        return pltpu.make_async_copy(counts_ref.at[k], matrix.at[slot], matrix_sem.at[slot])

    matrix_load(0).start()
    item_rows = items_tile.shape[1]
    item_tiles = items_ref.shape[0] // item_rows

    def items_load(t):
        slot = lax.rem(t, 2)
        return pltpu.make_async_copy(
            items_ref.at[pl.ds(t * item_rows, item_rows)], items_tile.at[slot], items_sem.at[slot]
        )

    items_load(0).start()
    barrier = pltpu.get_barrier_semaphore()
    for i in range(1, qrys):
        pl.semaphore_signal(
            barrier, inc=1, device_id=(n, lax.rem(q + i, qrys)), device_id_type=MESH
        )
    for i in range(1, parts):
        pl.semaphore_signal(
            barrier, inc=1, device_id=(lax.rem(n + i, parts), q), device_id_type=MESH
        )
    pl.semaphore_wait(barrier, qrys + parts - 2)

    def hop(k, h):
        axis, step = HOPS[k][1]
        if axis == 0:
            to = lax.rem(x + step + SIDE, SIDE) * SIDE + y
        else:
            to = x * SIDE + lax.rem(y + step + SIDE, SIDE)
        rows = pl.ds(h * half, half)
        source = summed.at[k, rows]
        return pltpu.make_async_remote_copy(
            src_ref=source, dst_ref=landed.at[k, rows],
            send_sem=block_send.at[k, h], recv_sem=block_recv.at[k, h],
            device_id=(to, q), device_id_type=MESH,
        )

    up = (n, lax.rem(z + 1, qrys // 2) * 2 + core)
    down = (n, lax.rem(z + qrys // 2 - 1, qrys // 2) * 2 + core)
    partner = (n, z * 2 + 1 - core)
    below, above = down[1], up[1]
    across = lax.rem(z + 2, qrys // 2) * 2 + core

    def spread(k, block, part, to, source=None):
        rows = pl.ds(0, own_rows) if part is None else pl.ds(part * (own_rows // 2), own_rows // 2)
        return pltpu.make_async_remote_copy(
            src_ref=gathered.at[block, rows] if source is None else source,
            dst_ref=gathered.at[block, rows],
            send_sem=query_send.at[k], recv_sem=query_recv.at[k],
            device_id=to, device_id_type=MESH,
        )

    spreads = [
        spread(0, q, None, up, queries_ref),
        spread(1, q, None, down, queries_ref),
        spread(2, q, None, partner, queries_ref),
        spread(3, below, 0, up),
        spread(4, above, 1, down),
        spread(5, below, None, partner),
        spread(6, above, None, partner),
        spread(7, across, 0, partner),
        spread(8, across, 1, partner),
    ]

    hops = {(k, h): hop(k, h) for k in range(len(HOPS) - 1) for h in range(2)}
    for k in range(3):
        spreads[k].start()
    wide = jnp.broadcast_to(log_ref[...], (8, count))
    column_ref[...] = jnp.transpose(wide)[:, 0:1]

    step = 64

    def table(t, _):
        items_load(t).wait()

        @pl.when(t + 1 < item_tiles)
        def _():
            items_load(t + 1).start()

        rows = items_tile[lax.rem(t, 2)]
        message = jnp.dot(rows, mw_ref[...], preferred_element_type=jnp.float32) + mb_ref[...]
        message = jnp.maximum(message, 0.0).astype(jnp.bfloat16)
        u = jnp.dot(message, nw_ref[...], preferred_element_type=jnp.float32)
        v = jnp.dot(rows, sw_ref[...], preferred_element_type=jnp.float32)
        for j in range(4):
            cols = slice(128 * j, 128 * j + 128)
            u_ref[pl.ds(t * item_rows * 4 + j, item_rows, stride=4), :] = u[:, cols]
            v_ref[pl.ds(t * item_rows * 4 + j, item_rows, stride=4), :] = v[:, cols]
        return 0

    v_ref[pl.ds(4 * items_ref.shape[0], 8), :] = jnp.zeros((8, 128), jnp.float32)
    lax.fori_loop(0, item_tiles, table, 0)
    unroll = 16
    u_rows = u_ref.reshape(u_ref.shape[0] // 4, 4, 128)
    v_rows = v_ref.reshape(v_ref.shape[0] // 4, 4, 128)

    def compute(k):
        def fetch(t, _):
            base = k * cap + t * unroll
            for s in range(unroll):
                g_ref[pl.ds(pl.multiple_of((t * unroll + s) * 4, 4), 4), :] = u_rows[fetch_ref[base + s]]
            return 0

        def own(t, _):
            own_base = k * count + t * unroll
            for s in range(unroll):
                z_ref[pl.ds(pl.multiple_of((t * unroll + s) * 4, 4), 4), :] = v_rows[self_ref[own_base + s]]
            return 0

        lax.fori_loop(0, cap // unroll, fetch, 0)
        lax.fori_loop(0, count // unroll, own, 0)
        matrix_load(k).wait()

        @pl.when(k + 1 < len(HOPS))
        def _():
            matrix_load(k + 1).start()

        rows = jnp.concatenate(
            [g_ref[pl.ds(j, cap, stride=4), :].astype(jnp.bfloat16) for j in range(4)], axis=1
        )
        for h in range(2):
            at = slice(h * half, h * half + half)
            mean = lax.dot_general(
                matrix[lax.rem(k, 2), :, at], rows, (((0,), (0,)), ((), ())),
                preferred_element_type=jnp.float32,
            )
            for j in range(4):
                cols = slice(128 * j, 128 * j + 128)
                own_part = z_ref[pl.ds(h * half * 4 + j, half, stride=4), :]
                summed[k, at, cols] = (mean[:, cols] + own_part).astype(jnp.bfloat16)

    def form(k, h):
        for child in CHILDREN[k]:
            hops[child, h].wait_recv()

        def body(t, _):
            rows = pl.ds(pl.multiple_of(h * half + t * step, step), step)
            total = summed[k, rows, :].astype(jnp.float32)
            for child in CHILDREN[k]:
                total = total + landed[child, rows, :].astype(jnp.float32)
            if HOPS[k][1] is None:
                hidden = jnp.maximum(total + bias_ref[...], 0.0)
                mean = jnp.mean(hidden * hidden, axis=-1, keepdims=True)
                negative_ref[rows, :] = (hidden * lax.rsqrt(mean + 0.25)).astype(jnp.bfloat16)
            else:
                summed[k, rows, :] = total.astype(jnp.bfloat16)
            return 0

        lax.fori_loop(0, half // step, body, 0)

    def after(k):
        if k == NEAR:
            spreads[0].wait_recv()
            spreads[3].start()
            spreads[5].start()
            spreads[1].wait_recv()
            spreads[4].start()
            spreads[6].start()
        if k == FAR:
            spreads[3].wait_recv()
            spreads[7].start()
            spreads[4].wait_recv()
            spreads[8].start()
        for h in range(2):
            if CHILDREN[k]:
                form(k, h)
            if HOPS[k][1] is not None:
                hops[k, h].start()

    def block(k, _):
        compute(k)
        for i in range(len(HOPS)):
            pl.when(k == i)(functools.partial(after, i))
        return 0

    lax.fori_loop(0, len(HOPS), block, 0)
    for k in (2, 5, 6, 7, 8):
        spreads[k].wait_recv()

    tile = own_rows // 2

    def score(block, h):
        cols = slice(h * tile, h * tile + tile)
        scores = lax.dot_general(
            negative_ref[...], matrix[h, 0:tile, :], (((1,), (1,)), ((), ())),
            preferred_element_type=jnp.float32,
        )
        scores = 0.25 * scores - column_ref[...]
        peak = jnp.max(scores, axis=0, keepdims=True)
        partial[block, 0:1, cols] = peak
        partial[block, 1:2, cols] = jnp.sum(jnp.exp(scores - peak), axis=0, keepdims=True)

    def tile_load(i, h):
        rows = pl.ds(h * tile, tile)
        source = queries_ref.at[rows] if i is None else gathered.at[lax.rem(q + i, qrys), rows]
        return pltpu.make_async_copy(source, matrix.at[h, pl.ds(0, tile)], tile_sem.at[h])

    def tile_start(i, h):
        @pl.when(i < qrys)
        def _():
            tile_load(i, h).start()

        @pl.when(i == qrys)
        def _():
            tile_load(None, h).start()

    for h in range(2):
        tile_load(1, h).start()

    def first(i):
        to = lax.rem(q + i, qrys)
        return pltpu.make_async_remote_copy(
            src_ref=partial.at[to], dst_ref=first_in.at[i],
            send_sem=first_send.at[i], recv_sem=first_recv.at[i],
            device_id=(n, to), device_id_type=MESH,
        )

    def each(i, _):
        for h in range(2):
            tile_load(None, h).wait()
            score(lax.rem(q + i, qrys), h)
            tile_start(i + 1, h)

        @pl.when(i > 1)
        def _():
            first(i - 1).start()

        return 0

    lax.fori_loop(1, qrys + 1, each, 0)
    peak, total = partial[q, 0:1, :], partial[q, 1:2, :]
    for i in range(1, qrys):
        first(i).wait_recv()
        peak, total = join(peak, total, first_in[i, 0:1, :], first_in[i, 1:2, :])
    second_out[0:1, :] = peak
    second_out[1:2, :] = total

    def second(i):
        return pltpu.make_async_remote_copy(
            src_ref=second_out, dst_ref=second_in.at[i],
            send_sem=second_send.at[i], recv_sem=second_recv.at[i],
            device_id=(lax.rem(n + i, parts), q), device_id_type=MESH,
        )

    for i in range(1, parts):
        second(i).start()
    for k in range(len(HOPS) - 1):
        for h in range(2):
            hops[k, h].wait_send()
    for k in range(9):
        spreads[k].wait_send()
    for i in range(1, qrys):
        first(i).wait_send()
    for i in range(1, parts):
        second(i).wait_recv()
        peak, total = join(peak, total, second_in[i, 0:1, :], second_in[i, 1:2, :])
    lse_ref[...] = peak + jnp.log(total) - math.log(count * parts * qrys)
    for i in range(1, parts):
        second(i).wait_send()


def tower(fetch, selves, counts, items, weights, bias, log_count, queries, qrys):
    parts, cap, count = counts.shape
    own_rows, width = queries.shape
    vmem = pl.BlockSpec(memory_space=pltpu.VMEM)
    smem = pl.BlockSpec(memory_space=pltpu.SMEM)
    hbm = pl.BlockSpec(memory_space=pltpu.HBM)
    dma = pltpu.SemaphoreType.DMA
    hops = len(HOPS) - 1
    return pl.pallas_call(
        functools.partial(tower_kernel, parts, qrys),
        in_specs=[smem, smem, hbm, hbm, vmem, vmem, vmem, vmem, vmem, vmem, hbm],
        out_specs=(vmem, vmem, hbm),
        out_shape=(
            jax.ShapeDtypeStruct((count, width), jnp.bfloat16),
            jax.ShapeDtypeStruct((1, own_rows), jnp.float32),
            jax.ShapeDtypeStruct((qrys, own_rows, width), jnp.bfloat16),
        ),
        scratch_shapes=[
            pltpu.VMEM((4 * items.shape[0], 128), jnp.float32),
            pltpu.VMEM((4 * items.shape[0] + 8, 128), jnp.float32),
            pltpu.VMEM((2, 512, width), jnp.bfloat16),
            pltpu.VMEM((hops, count, width), jnp.bfloat16),
            pltpu.VMEM((hops + 1, count, width), jnp.bfloat16),
            pltpu.VMEM((2, cap, count), jnp.bfloat16),
            pltpu.VMEM((4 * cap, 128), jnp.float32),
            pltpu.VMEM((4 * count, 128), jnp.float32),
            pltpu.VMEM((count, 1), jnp.float32),
            pltpu.VMEM((qrys, 2, own_rows), jnp.float32),
            pltpu.VMEM((qrys, 2, own_rows), jnp.float32),
            pltpu.VMEM((2, own_rows), jnp.float32),
            pltpu.VMEM((parts, 2, own_rows), jnp.float32),
            dma((2,)), dma((2,)), dma((2,)), dma((hops, 2)), dma((hops, 2)), dma((9,)), dma((9,)),
            dma((qrys,)), dma((qrys,)), dma((parts,)), dma((parts,)),
        ],
        name="tower",
        compiler_params=pltpu.CompilerParams(
            collective_id=0, has_side_effects=True, vmem_limit_bytes=TOWER_VMEM
        ),
    )(fetch, selves, counts, items, *weights, bias, log_count, queries)


def per_device(
    items_table,
    fetch_rows,
    neighbour_slots,
    neighbour_count,
    self_slot,
    negative_count,
    message_weight,
    message_bias,
    self_weight,
    neighbour_weight,
    output_bias,
    queries,
):
    parts, cap = fetch_rows.shape
    count, neighbours = neighbour_slots.shape

    slots = neighbour_slots.T
    live = jnp.arange(neighbours, dtype=jnp.int32)[:, None] < neighbour_count[None, :]
    owner = slots // cap
    local = slots - owner * cap
    found, counts = compact(jnp.where(live, owner, -1), local, parts)
    most = jnp.max(counts.reshape(parts, count // 128, 128), axis=2)
    self_row = fetch_rows.reshape(-1)[self_slot]
    mine = self_slot[None, :] // cap == jnp.arange(parts, dtype=jnp.int32)[:, None]
    self_local = jnp.where(mine, self_row[None, :], items_table.shape[0])
    rest = jnp.concatenate(
        [
            self_local,
            jnp.broadcast_to(neighbour_count[None, :], (parts, count)),
            jnp.pad(most, ((0, 0), (0, count - most.shape[1]))),
            jnp.pad(fetch_rows, ((0, 0), (0, (ROWS - neighbours - 3) * count - cap))),
        ],
        axis=1,
    ).astype(jnp.int16)
    slab = jnp.concatenate(
        [found.transpose(1, 0, 2), rest.reshape(parts, ROWS - neighbours, count)], axis=1
    )
    slab = lax.all_to_all(slab, "neg", split_axis=0, concat_axis=0, tiled=True)

    rest = slab[:, neighbours:].astype(jnp.int32)
    most_in = rest[:, 2, : count // 128][:, None, :]

    here = lax.axis_index("neg")
    x, y = here // SIDE, here % SIDE
    ns = [((x + dx) % SIDE) * SIDE + (y + dy) % SIDE for (dx, dy), _ in HOPS]
    qry = lax.axis_index("qry")
    own_count = lax.dynamic_slice_in_dim(negative_count, qry * count, count)
    log_count = jnp.log(own_count.astype(jnp.float32))[None, :]

    ns = jnp.stack(ns)
    ordered = rest[ns]
    self_in = ordered[:, 0].reshape(-1)
    fetch_in = ordered[:, 3:5].reshape(parts, -1)[:, :cap].reshape(-1)
    matrices = counts_blocks(ns, most_in, slab, cap)
    matrices = pltpu.with_memory_space_constraint(matrices, pltpu.HBM)
    negative_embed, query_lse, _ = tower(
        fetch_in, self_in, matrices, items_table,
        (message_weight, message_bias[None], neighbour_weight, self_weight),
        output_bias[None], log_count, queries,
        lax.axis_size("qry"),
    )
    return (negative_embed, query_lse[0])


def solution(mesh):
    in_specs = (
        P("neg", None),
        P(("neg", "qry"), None),
        P(("neg", "qry"), None),
        P(("neg", "qry")),
        P(("neg", "qry")),
        P("neg"),
        P(),
        P(),
        P(),
        P(),
        P(),
        P("qry", None),
    )
    out_specs = (P(("neg", "qry"), None), P("qry"))
    return jax.shard_map(
        per_device, mesh=mesh, in_specs=in_specs, out_specs=out_specs, check_vma=False
    )
```

```python
import functools
import math

import jax
import jax.numpy as jnp
from jax import lax
from jax.experimental import pallas as pl
from jax.experimental.pallas import tpu as pltpu
from jax.sharding import PartitionSpec as P


SIDE = 4
HOPS = (
    ((2, 2), (0, 1)),
    ((2, 1), (0, -1)),
    ((3, 2), (1, 1)),
    ((2, 0), (0, 1)),
    ((1, 2), (1, -1)),
    ((2, 3), (0, -1)),
    ((0, 2), (1, 1)),
    ((1, 1), (0, 1)),
    ((3, 1), (1, 1)),
    ((1, 3), (1, -1)),
    ((3, 3), (0, -1)),
    ((1, 0), (0, 1)),
    ((0, 1), (1, 1)),
    ((0, 3), (1, -1)),
    ((3, 0), (0, -1)),
    ((0, 0), None),
)
PLACE = {offset: k for k, (offset, _) in enumerate(HOPS)}
CHILDREN = [[] for _ in HOPS]
for _k, ((_dx, _dy), _way) in enumerate(HOPS):
    if _way is not None:
        _to = ((_dx - _way[1]) % SIDE, _dy) if _way[0] == 0 else (_dx, (_dy - _way[1]) % SIDE)
        CHILDREN[PLACE[_to]].append(_k)
NEAR, FAR = 4, 10
TOWER_VMEM = 62 * 2**20
WORDS = 2048
ITEM_ROWS = 8192
MESH = pl.DeviceIdType.MESH


def prepare_kernel(
    slots_ref, count_ref, self_ref, fetch_ref, slab_ref, words_ref, owner_ref, local_ref, table_ref
):
    neighbours, width = slots_ref.shape
    parts, cap = fetch_ref.shape

    slots = slots_ref[...]
    owner = ((slots.astype(jnp.float32) + 0.5) * (1.0 / cap)).astype(jnp.int32)
    order = lax.broadcasted_iota(jnp.int32, (neighbours, width), 0)
    local_ref[...] = slots - owner * cap
    owner_ref[...] = jnp.where(order < count_ref[...], owner, -1)

    for i in range(cap // 128):
        rows = fetch_ref[:, 128 * i : 128 * i + 128]
        table_ref[pl.ds(i, parts, stride=cap // 128), :] = rows
        words_ref[pl.ds(i, parts, stride=WORDS // 128), :] = rows
    chunks = parts * cap // 128
    own = self_ref[...]
    high = lax.shift_right_logical(own, 7)
    low = own - lax.shift_left(high, 7)
    pick = (lax.broadcasted_iota(jnp.int32, (chunks, width), 0) == high).astype(jnp.float32)
    pick = pick.astype(jnp.bfloat16)
    rows = table_ref[...]
    upper = lax.shift_right_logical(rows, 7)
    lower = rows - lax.shift_left(upper, 7)
    found = [
        lax.dot_general(
            part.astype(jnp.float32).astype(jnp.bfloat16), pick, (((0,), (0,)), ((), ())),
            preferred_element_type=jnp.float32,
        )
        for part in (upper, lower)
    ]
    at = lax.broadcasted_iota(jnp.int32, (128, width), 0) == low
    own_row = jnp.sum(jnp.where(at, 128.0 * found[0] + found[1], 0.0), axis=0, keepdims=True)
    own_owner = ((own.astype(jnp.float32) + 0.5) * (1.0 / cap)).astype(jnp.int32)
    mine = lax.broadcasted_iota(jnp.int32, (parts, width), 0) == own_owner
    own_rows = jnp.where(mine, own_row.astype(jnp.int32), ITEM_ROWS)
    for i in range(width // 128):
        words_ref[pl.ds(cap // 128 + i, parts, stride=WORDS // 128), :] = own_rows[
            :, 128 * i : 128 * i + 128
        ]
    slab_ref[:, neighbours:, :] = jnp.broadcast_to(
        count_ref[...][None], (parts, slab_ref.shape[1] - neighbours, width)
    ).astype(jnp.int16)

    part = lax.broadcasted_iota(jnp.int32, (parts, 128), 0).astype(jnp.int16)
    one = jnp.ones((parts, 128), jnp.int16)
    zero = jnp.zeros((parts, 128), jnp.int16)
    lane = lax.broadcasted_iota(jnp.int32, (parts, 128), 1)
    most = jnp.zeros((parts, 128), jnp.int32)
    for t in range(width // 128):
        lanes = slice(128 * t, 128 * t + 128)
        seen = zero
        found = [zero - one] * neighbours
        for k in range(neighbours):
            owner = jnp.broadcast_to(owner_ref[k : k + 1, lanes], (parts, 128)).astype(jnp.int16)
            local = jnp.broadcast_to(local_ref[k : k + 1, lanes], (parts, 128)).astype(jnp.int16)
            mine = owner == part
            rank = jnp.where(mine, seen, zero - one)
            for j in range(k + 1):
                found[j] = jnp.where(rank == jnp.int16(j), local, found[j])
            seen = seen + jnp.where(mine, one, zero)
        for j in range(neighbours):
            slab_ref[:, j, lanes] = found[j]
        peak = jnp.max(seen.astype(jnp.int32), axis=1, keepdims=True)
        most = jnp.where(lane == t, peak, most)
    words_ref[pl.ds((cap + width) // 128, parts, stride=WORDS // 128), :] = most


def prepare(slots, count, own, fetch):
    neighbours, width = slots.shape
    parts, cap = fetch.shape
    return pl.pallas_call(
        prepare_kernel,
        out_shape=(
            jax.ShapeDtypeStruct((parts, neighbours + 8, width), jnp.int16),
            jax.ShapeDtypeStruct((parts * WORDS // 128, 128), jnp.int32),
        ),
        scratch_shapes=[
            pltpu.VMEM((neighbours, width), jnp.int32),
            pltpu.VMEM((neighbours, width), jnp.int32),
            pltpu.VMEM((parts * cap // 128, 128), jnp.int32),
        ],
        name="prepare",
        compiler_params=pltpu.CompilerParams(vmem_limit_bytes=16 * 2**20),
    )(slots, count[None], own[None], fetch)


def exchange_kernel(
    slab_ref, words_ref, slab_out, words_out, slab_send, slab_recv, words_send, words_recv, own_sem
):
    n, q = lax.axis_index("neg"), lax.axis_index("qry")
    x, y = n // SIDE, n % SIDE
    lines = WORDS // 128
    last = len(HOPS) - 1

    def target(k):
        dx, dy = HOPS[k][0]
        return lax.rem(x + SIDE - dx, SIDE) * SIDE + lax.rem(y + SIDE - dy, SIDE)

    barrier = pltpu.get_barrier_semaphore()
    for k in range(last):
        pl.semaphore_signal(barrier, inc=1, device_id=(target(k), q), device_id_type=MESH)
    pl.semaphore_wait(barrier, last)

    copies = []
    for k in range(last):
        to = target(k)
        for source, out, send, recv, at in (
            (slab_ref.at[to], slab_out.at[k], slab_send, slab_recv, None),
            (
                words_ref.at[pl.ds(to * lines, lines)], words_out.at[pl.ds(k * lines, lines)],
                words_send, words_recv, None,
            ),
        ):
            copies.append(
                pltpu.make_async_remote_copy(
                    src_ref=source, dst_ref=out, send_sem=send.at[k], recv_sem=recv.at[k],
                    device_id=(to, q), device_id_type=MESH,
                )
            )
            copies[-1].start()
    own = [
        pltpu.make_async_copy(slab_ref.at[n], slab_out.at[last], own_sem.at[0]),
        pltpu.make_async_copy(
            words_ref.at[pl.ds(n * lines, lines)], words_out.at[pl.ds(last * lines, lines)],
            own_sem.at[1],
        ),
    ]
    for copy in own:
        copy.start()
    for copy in own:
        copy.wait()
    for copy in copies:
        copy.wait_recv()
    for copy in copies:
        copy.wait_send()


def exchange(slab, words):
    vmem = pl.BlockSpec(memory_space=pltpu.VMEM)
    dma = pltpu.SemaphoreType.DMA
    hops = len(HOPS) - 1
    return pl.pallas_call(
        exchange_kernel,
        in_specs=[vmem, vmem],
        out_specs=(vmem, vmem),
        out_shape=(
            jax.ShapeDtypeStruct(slab.shape, slab.dtype),
            jax.ShapeDtypeStruct(words.shape, words.dtype),
        ),
        scratch_shapes=[dma((hops,)), dma((hops,)), dma((hops,)), dma((hops,)), dma((2,))],
        name="exchange",
        compiler_params=pltpu.CompilerParams(
            collective_id=1, has_side_effects=True, vmem_limit_bytes=8 * 2**20
        ),
    )(slab, words)


def counts_kernel(words_ref, slab_ref, out_ref):
    cap, count = out_ref.shape[1:]
    neighbours = slab_ref.shape[1] - 8
    tile = 16
    row = lax.broadcasted_iota(jnp.int32, (tile, 128), 0).astype(jnp.int16)
    zero = jnp.zeros((tile, 128), jnp.bfloat16)

    def build(t, _):
        lanes = pl.ds(pl.multiple_of(t * 128, 128), 128)
        rows = slab_ref[0, :, lanes].astype(jnp.int32)
        most = words_ref[pl.program_id(0) * WORDS + cap + count + t]
        scale = 1.0 / rows[neighbours + 1 : neighbours + 2].astype(jnp.float32)
        scale = jnp.broadcast_to(scale, (tile, 128)).astype(jnp.bfloat16)

        def spread(k):
            return jnp.broadcast_to(rows[k : k + 1], (tile, 128)).astype(jnp.int16)

        slots = [spread(k) for k in range(6)]
        for i in range(cap // tile):
            here = row + jnp.int16(i * tile)
            total = jnp.where(slots[0] == here, scale, zero)
            for slot in slots[1:]:
                total = total + jnp.where(slot == here, scale, zero)
            out_ref[0, i * tile : (i + 1) * tile, lanes] = total

        def more(first, step):
            if first >= neighbours:
                return

            @pl.when(most > first)
            def _():
                last = min(first + step, neighbours)
                slots = [spread(k) for k in range(first, last)]

                def body(i, _):
                    at = pl.ds(pl.multiple_of(i * tile, tile), tile)
                    here = row + (i * tile).astype(jnp.int16)
                    total = out_ref[0, at, lanes]
                    for slot in slots:
                        total = total + jnp.where(slot == here, scale, zero)
                    out_ref[0, at, lanes] = total
                    return 0

                lax.fori_loop(0, cap // tile, body, 0, unroll=first < 8)
                more(last, 2 * step)

        more(6, 2)
        return 0

    lax.fori_loop(0, count // 128, build, 0)


def counts_blocks(words, slab, cap):
    parts, rows, count = slab.shape
    return pl.pallas_call(
        counts_kernel,
        grid=(parts,),
        in_specs=[
            pl.BlockSpec(memory_space=pltpu.SMEM),
            pl.BlockSpec((1, rows, count), lambda i: (i, 0, 0)),
        ],
        out_specs=pl.BlockSpec((1, cap, count), lambda i: (i, 0, 0)),
        out_shape=pltpu.HBM((parts, cap, count), jnp.bfloat16),
        name="counts",
        cost_estimate=pl.CostEstimate(
            flops=10**9, bytes_accessed=12 * 2**20, transcendentals=0
        ),
        compiler_params=pltpu.CompilerParams(vmem_limit_bytes=6 * 2**20),
    )(words, slab)


def join(peak, total, other_peak, other_total):
    top = jnp.maximum(peak, other_peak)
    return top, total * jnp.exp(peak - top) + other_total * jnp.exp(other_peak - top)


def tower_kernel(
    parts, qrys, words_ref, counts_ref, items_ref, mw_ref, mb_ref, nw_ref,
    sw_ref, bias_ref, log_ref, queries_ref, negative_ref, lse_ref, gathered,
    u_ref, v_ref, items_tile, landed, summed, matrix, g_ref, z_ref, column_ref, partial, first_in,
    second_out, second_in, items_sem, matrix_sem, tile_sem, block_send, block_recv, query_send,
    query_recv, first_send, first_recv, second_send, second_recv,
):
    n, q = lax.axis_index("neg"), lax.axis_index("qry")
    x, y = n // SIDE, n % SIDE
    z, core = q // 2, q % 2
    cap, count = counts_ref.shape[1:]
    own_rows = queries_ref.shape[0]
    half = count // 2

    def matrix_load(k):
        slot = lax.rem(k, 2)
        return pltpu.make_async_copy(counts_ref.at[k], matrix.at[slot], matrix_sem.at[slot])

    matrix_load(0).start()
    item_rows = items_tile.shape[1]
    item_tiles = items_ref.shape[0] // item_rows

    def items_load(t):
        slot = lax.rem(t, 2)
        return pltpu.make_async_copy(
            items_ref.at[pl.ds(t * item_rows, item_rows)], items_tile.at[slot], items_sem.at[slot]
        )

    items_load(0).start()
    barrier = pltpu.get_barrier_semaphore()
    for i in range(1, qrys):
        pl.semaphore_signal(
            barrier, inc=1, device_id=(n, lax.rem(q + i, qrys)), device_id_type=MESH
        )
    for i in range(1, parts):
        pl.semaphore_signal(
            barrier, inc=1, device_id=(lax.rem(n + i, parts), q), device_id_type=MESH
        )
    pl.semaphore_wait(barrier, qrys + parts - 2)

    def hop(k, h):
        axis, step = HOPS[k][1]
        if axis == 0:
            to = lax.rem(x + step + SIDE, SIDE) * SIDE + y
        else:
            to = x * SIDE + lax.rem(y + step + SIDE, SIDE)
        rows = pl.ds(h * half, half)
        source = summed.at[k, rows]
        return pltpu.make_async_remote_copy(
            src_ref=source, dst_ref=landed.at[k, rows],
            send_sem=block_send.at[k, h], recv_sem=block_recv.at[k, h],
            device_id=(to, q), device_id_type=MESH,
        )

    up = (n, lax.rem(z + 1, qrys // 2) * 2 + core)
    down = (n, lax.rem(z + qrys // 2 - 1, qrys // 2) * 2 + core)
    partner = (n, z * 2 + 1 - core)
    below, above = down[1], up[1]
    across = lax.rem(z + 2, qrys // 2) * 2 + core

    def spread(k, block, part, to, source=None):
        rows = pl.ds(0, own_rows) if part is None else pl.ds(part * (own_rows // 2), own_rows // 2)
        return pltpu.make_async_remote_copy(
            src_ref=gathered.at[block, rows] if source is None else source,
            dst_ref=gathered.at[block, rows],
            send_sem=query_send.at[k], recv_sem=query_recv.at[k],
            device_id=to, device_id_type=MESH,
        )

    spreads = [
        spread(0, q, None, up, queries_ref),
        spread(1, q, None, down, queries_ref),
        spread(2, q, None, partner, queries_ref),
        spread(3, below, 0, up),
        spread(4, above, 1, down),
        spread(5, below, None, partner),
        spread(6, above, None, partner),
        spread(7, across, 0, partner),
        spread(8, across, 1, partner),
    ]

    hops = {(k, h): hop(k, h) for k in range(len(HOPS) - 1) for h in range(2)}
    for k in range(3):
        spreads[k].start()
    wide = jnp.broadcast_to(log_ref[...], (8, count))
    column_ref[...] = jnp.transpose(wide)[:, 0:1]

    step = 64

    def table(t, _):
        items_load(t).wait()

        @pl.when(t + 1 < item_tiles)
        def _():
            items_load(t + 1).start()

        rows = items_tile[lax.rem(t, 2)]
        message = jnp.dot(rows, mw_ref[...], preferred_element_type=jnp.float32) + mb_ref[...]
        message = jnp.maximum(message, 0.0).astype(jnp.bfloat16)
        u = jnp.dot(message, nw_ref[...], preferred_element_type=jnp.float32)
        v = jnp.dot(rows, sw_ref[...], preferred_element_type=jnp.float32)
        for j in range(4):
            cols = slice(128 * j, 128 * j + 128)
            u_ref[pl.ds(t * item_rows * 4 + j, item_rows, stride=4), :] = u[:, cols]
            v_ref[pl.ds(t * item_rows * 4 + j, item_rows, stride=4), :] = v[:, cols]
        return 0

    v_ref[pl.ds(4 * items_ref.shape[0], 8), :] = jnp.zeros((8, 128), jnp.float32)
    lax.fori_loop(0, item_tiles, table, 0)
    unroll = 16
    u_rows = u_ref.reshape(u_ref.shape[0] // 4, 4, 128)
    v_rows = v_ref.reshape(v_ref.shape[0] // 4, 4, 128)

    def compute(k):
        def fetch(t, _):
            base = k * WORDS + t * unroll
            for s in range(unroll):
                g_ref[pl.ds(pl.multiple_of((t * unroll + s) * 4, 4), 4), :] = u_rows[words_ref[base + s]]
            return 0

        def own(t, _):
            own_base = k * WORDS + cap + t * unroll
            for s in range(unroll):
                z_ref[pl.ds(pl.multiple_of((t * unroll + s) * 4, 4), 4), :] = v_rows[words_ref[own_base + s]]
            return 0

        lax.fori_loop(0, cap // unroll, fetch, 0)
        lax.fori_loop(0, count // unroll, own, 0)
        matrix_load(k).wait()

        @pl.when(k + 1 < len(HOPS))
        def _():
            matrix_load(k + 1).start()

        rows = jnp.concatenate(
            [g_ref[pl.ds(j, cap, stride=4), :].astype(jnp.bfloat16) for j in range(4)], axis=1
        )
        for h in range(2):
            at = slice(h * half, h * half + half)
            mean = lax.dot_general(
                matrix[lax.rem(k, 2), :, at], rows, (((0,), (0,)), ((), ())),
                preferred_element_type=jnp.float32,
            )
            for j in range(4):
                cols = slice(128 * j, 128 * j + 128)
                own_part = z_ref[pl.ds(h * half * 4 + j, half, stride=4), :]
                summed[k, at, cols] = (mean[:, cols] + own_part).astype(jnp.bfloat16)

    def form(k, h):
        for child in CHILDREN[k]:
            hops[child, h].wait_recv()

        def body(t, _):
            rows = pl.ds(pl.multiple_of(h * half + t * step, step), step)
            total = summed[k, rows, :].astype(jnp.float32)
            for child in CHILDREN[k]:
                total = total + landed[child, rows, :].astype(jnp.float32)
            if HOPS[k][1] is None:
                hidden = jnp.maximum(total + bias_ref[...], 0.0)
                mean = jnp.mean(hidden * hidden, axis=-1, keepdims=True)
                negative_ref[rows, :] = (hidden * lax.rsqrt(mean + 0.25)).astype(jnp.bfloat16)
            else:
                summed[k, rows, :] = total.astype(jnp.bfloat16)
            return 0

        lax.fori_loop(0, half // step, body, 0)

    def after(k):
        if k == NEAR:
            spreads[0].wait_recv()
            spreads[3].start()
            spreads[5].start()
            spreads[1].wait_recv()
            spreads[4].start()
            spreads[6].start()
        if k == FAR:
            spreads[3].wait_recv()
            spreads[7].start()
            spreads[4].wait_recv()
            spreads[8].start()
        for h in range(2):
            if CHILDREN[k]:
                form(k, h)
            if HOPS[k][1] is not None:
                hops[k, h].start()

    def block(k, _):
        compute(k)
        for i in range(len(HOPS)):
            pl.when(k == i)(functools.partial(after, i))
        return 0

    lax.fori_loop(0, len(HOPS), block, 0)
    for k in (2, 5, 6, 7, 8):
        spreads[k].wait_recv()

    tile = own_rows // 2

    def score(block, h):
        cols = slice(h * tile, h * tile + tile)
        scores = lax.dot_general(
            negative_ref[...], matrix[h, 0:tile, :], (((1,), (1,)), ((), ())),
            preferred_element_type=jnp.float32,
        )
        scores = 0.25 * scores - column_ref[...]
        peak = jnp.max(scores, axis=0, keepdims=True)
        partial[block, 0:1, cols] = peak
        partial[block, 1:2, cols] = jnp.sum(jnp.exp(scores - peak), axis=0, keepdims=True)

    def tile_load(i, h):
        rows = pl.ds(h * tile, tile)
        source = queries_ref.at[rows] if i is None else gathered.at[lax.rem(q + i, qrys), rows]
        return pltpu.make_async_copy(source, matrix.at[h, pl.ds(0, tile)], tile_sem.at[h])

    def tile_start(i, h):
        @pl.when(i < qrys)
        def _():
            tile_load(i, h).start()

        @pl.when(i == qrys)
        def _():
            tile_load(None, h).start()

    for h in range(2):
        tile_load(1, h).start()

    def first(i):
        to = lax.rem(q + i, qrys)
        return pltpu.make_async_remote_copy(
            src_ref=partial.at[to], dst_ref=first_in.at[i],
            send_sem=first_send.at[i], recv_sem=first_recv.at[i],
            device_id=(n, to), device_id_type=MESH,
        )

    def each(i, _):
        for h in range(2):
            tile_load(None, h).wait()
            score(lax.rem(q + i, qrys), h)
            tile_start(i + 1, h)

        @pl.when(i > 1)
        def _():
            first(i - 1).start()

        return 0

    lax.fori_loop(1, qrys + 1, each, 0)
    peak, total = partial[q, 0:1, :], partial[q, 1:2, :]
    for i in range(1, qrys):
        first(i).wait_recv()
        peak, total = join(peak, total, first_in[i, 0:1, :], first_in[i, 1:2, :])
    second_out[0:1, :] = peak
    second_out[1:2, :] = total

    def second(i):
        return pltpu.make_async_remote_copy(
            src_ref=second_out, dst_ref=second_in.at[i],
            send_sem=second_send.at[i], recv_sem=second_recv.at[i],
            device_id=(lax.rem(n + i, parts), q), device_id_type=MESH,
        )

    for i in range(1, parts):
        second(i).start()
    for k in range(len(HOPS) - 1):
        for h in range(2):
            hops[k, h].wait_send()
    for k in range(9):
        spreads[k].wait_send()
    for i in range(1, qrys):
        first(i).wait_send()
    for i in range(1, parts):
        second(i).wait_recv()
        peak, total = join(peak, total, second_in[i, 0:1, :], second_in[i, 1:2, :])
    lse_ref[...] = peak + jnp.log(total) - math.log(count * parts * qrys)
    for i in range(1, parts):
        second(i).wait_send()


def tower(words, counts, items, weights, bias, log_count, queries, qrys):
    parts, cap, count = counts.shape
    own_rows, width = queries.shape
    vmem = pl.BlockSpec(memory_space=pltpu.VMEM)
    smem = pl.BlockSpec(memory_space=pltpu.SMEM)
    hbm = pl.BlockSpec(memory_space=pltpu.HBM)
    dma = pltpu.SemaphoreType.DMA
    hops = len(HOPS) - 1
    return pl.pallas_call(
        functools.partial(tower_kernel, parts, qrys),
        in_specs=[smem, hbm, hbm, vmem, vmem, vmem, vmem, vmem, vmem, hbm],
        out_specs=(vmem, vmem, hbm),
        out_shape=(
            jax.ShapeDtypeStruct((count, width), jnp.bfloat16),
            jax.ShapeDtypeStruct((1, own_rows), jnp.float32),
            jax.ShapeDtypeStruct((qrys, own_rows, width), jnp.bfloat16),
        ),
        scratch_shapes=[
            pltpu.VMEM((4 * items.shape[0], 128), jnp.float32),
            pltpu.VMEM((4 * items.shape[0] + 8, 128), jnp.float32),
            pltpu.VMEM((2, 512, width), jnp.bfloat16),
            pltpu.VMEM((hops, count, width), jnp.bfloat16),
            pltpu.VMEM((hops + 1, count, width), jnp.bfloat16),
            pltpu.VMEM((2, cap, count), jnp.bfloat16),
            pltpu.VMEM((4 * cap, 128), jnp.float32),
            pltpu.VMEM((4 * count, 128), jnp.float32),
            pltpu.VMEM((count, 1), jnp.float32),
            pltpu.VMEM((qrys, 2, own_rows), jnp.float32),
            pltpu.VMEM((qrys, 2, own_rows), jnp.float32),
            pltpu.VMEM((2, own_rows), jnp.float32),
            pltpu.VMEM((parts, 2, own_rows), jnp.float32),
            dma((2,)), dma((2,)), dma((2,)), dma((hops, 2)), dma((hops, 2)), dma((9,)), dma((9,)),
            dma((qrys,)), dma((qrys,)), dma((parts,)), dma((parts,)),
        ],
        name="tower",
        compiler_params=pltpu.CompilerParams(
            collective_id=0, has_side_effects=True, vmem_limit_bytes=TOWER_VMEM
        ),
    )(words, counts, items, *weights, bias, log_count, queries)


def per_device(
    items_table,
    fetch_rows,
    neighbour_slots,
    neighbour_count,
    self_slot,
    negative_count,
    message_weight,
    message_bias,
    self_weight,
    neighbour_weight,
    output_bias,
    queries,
):
    parts, cap = fetch_rows.shape
    count, neighbours = neighbour_slots.shape

    assert items_table.shape[0] == ITEM_ROWS
    slab, words = prepare(neighbour_slots.T, neighbour_count, self_slot, fetch_rows)
    slab, words = exchange(slab, words)
    words = words.reshape(-1)

    qry = lax.axis_index("qry")
    own_count = lax.dynamic_slice_in_dim(negative_count, qry * count, count)
    log_count = jnp.log(own_count.astype(jnp.float32))[None, :]

    matrices = counts_blocks(words, slab, cap)
    matrices = pltpu.with_memory_space_constraint(matrices, pltpu.HBM)
    negative_embed, query_lse, _ = tower(
        words, matrices, items_table,
        (message_weight, message_bias[None], neighbour_weight, self_weight),
        output_bias[None], log_count, queries,
        lax.axis_size("qry"),
    )
    return (negative_embed, query_lse[0])


def solution(mesh):
    in_specs = (
        P("neg", None),
        P(("neg", "qry"), None),
        P(("neg", "qry"), None),
        P(("neg", "qry")),
        P(("neg", "qry")),
        P("neg"),
        P(),
        P(),
        P(),
        P(),
        P(),
        P("qry", None),
    )
    out_specs = (P(("neg", "qry"), None), P("qry"))
    return jax.shard_map(
        per_device, mesh=mesh, in_specs=in_specs, out_specs=out_specs, check_vma=False
    )
```

```python
import functools
import math

import jax
import jax.numpy as jnp
from jax import lax
from jax.experimental import pallas as pl
from jax.experimental.pallas import tpu as pltpu
from jax.sharding import PartitionSpec as P


SIDE = 4
HOPS = (
    ((2, 2), (0, 1)),
    ((2, 1), (0, -1)),
    ((3, 2), (1, 1)),
    ((2, 0), (0, 1)),
    ((1, 2), (1, -1)),
    ((2, 3), (0, -1)),
    ((0, 2), (1, 1)),
    ((1, 1), (0, 1)),
    ((3, 1), (1, 1)),
    ((1, 3), (1, -1)),
    ((3, 3), (0, -1)),
    ((1, 0), (0, 1)),
    ((0, 1), (1, 1)),
    ((0, 3), (1, -1)),
    ((3, 0), (0, -1)),
    ((0, 0), None),
)
PLACE = {offset: k for k, (offset, _) in enumerate(HOPS)}
CHILDREN = [[] for _ in HOPS]
for _k, ((_dx, _dy), _way) in enumerate(HOPS):
    if _way is not None:
        _to = ((_dx - _way[1]) % SIDE, _dy) if _way[0] == 0 else (_dx, (_dy - _way[1]) % SIDE)
        CHILDREN[PLACE[_to]].append(_k)
NEAR, FAR = 4, 10
TOWER_VMEM = 60 * 2**20
WORDS = 2048
ITEM_ROWS = 8192
MESH = pl.DeviceIdType.MESH


def prepare_kernel(
    slots_ref, count_ref, self_ref, fetch_ref, slab_ref, words_ref, owner_ref, local_ref, table_ref
):
    neighbours, width = slots_ref.shape
    parts, cap = fetch_ref.shape

    slots = slots_ref[...]
    owner = ((slots.astype(jnp.float32) + 0.5) * (1.0 / cap)).astype(jnp.int32)
    order = lax.broadcasted_iota(jnp.int32, (neighbours, width), 0)
    local_ref[...] = slots - owner * cap
    owner_ref[...] = jnp.where(order < count_ref[...], owner, -1)

    for i in range(cap // 128):
        rows = fetch_ref[:, 128 * i : 128 * i + 128]
        table_ref[pl.ds(i, parts, stride=cap // 128), :] = rows
        words_ref[pl.ds(i, parts, stride=WORDS // 128), :] = rows
    chunks = parts * cap // 128
    own = self_ref[...]
    high = lax.shift_right_logical(own, 7)
    low = own - lax.shift_left(high, 7)
    pick = (lax.broadcasted_iota(jnp.int32, (chunks, width), 0) == high).astype(jnp.float32)
    pick = pick.astype(jnp.bfloat16)
    rows = table_ref[...]
    upper = lax.shift_right_logical(rows, 7)
    lower = rows - lax.shift_left(upper, 7)
    found = [
        lax.dot_general(
            part.astype(jnp.float32).astype(jnp.bfloat16), pick, (((0,), (0,)), ((), ())),
            preferred_element_type=jnp.float32,
        )
        for part in (upper, lower)
    ]
    at = lax.broadcasted_iota(jnp.int32, (128, width), 0) == low
    own_row = jnp.sum(jnp.where(at, 128.0 * found[0] + found[1], 0.0), axis=0, keepdims=True)
    own_owner = ((own.astype(jnp.float32) + 0.5) * (1.0 / cap)).astype(jnp.int32)
    mine = lax.broadcasted_iota(jnp.int32, (parts, width), 0) == own_owner
    own_rows = jnp.where(mine, own_row.astype(jnp.int32), ITEM_ROWS)
    for i in range(width // 128):
        words_ref[pl.ds(cap // 128 + i, parts, stride=WORDS // 128), :] = own_rows[
            :, 128 * i : 128 * i + 128
        ]
    slab_ref[:, neighbours:, :] = jnp.broadcast_to(
        count_ref[...][None], (parts, slab_ref.shape[1] - neighbours, width)
    ).astype(jnp.int16)

    part = lax.broadcasted_iota(jnp.int32, (parts, 128), 0).astype(jnp.int16)
    one = jnp.ones((parts, 128), jnp.int16)
    zero = jnp.zeros((parts, 128), jnp.int16)
    lane = lax.broadcasted_iota(jnp.int32, (parts, 128), 1)
    most = jnp.zeros((parts, 128), jnp.int32)
    for t in range(width // 128):
        lanes = slice(128 * t, 128 * t + 128)
        seen = zero
        found = [zero - one] * neighbours
        for k in range(neighbours):
            owner = jnp.broadcast_to(owner_ref[k : k + 1, lanes], (parts, 128)).astype(jnp.int16)
            local = jnp.broadcast_to(local_ref[k : k + 1, lanes], (parts, 128)).astype(jnp.int16)
            mine = owner == part
            rank = jnp.where(mine, seen, zero - one)
            for j in range(k + 1):
                found[j] = jnp.where(rank == jnp.int16(j), local, found[j])
            seen = seen + jnp.where(mine, one, zero)
        for j in range(neighbours):
            slab_ref[:, j, lanes] = found[j]
        peak = jnp.max(seen.astype(jnp.int32), axis=1, keepdims=True)
        most = jnp.where(lane == t, peak, most)
    words_ref[pl.ds((cap + width) // 128, parts, stride=WORDS // 128), :] = most


def prepare(slots, count, own, fetch):
    neighbours, width = slots.shape
    parts, cap = fetch.shape
    return pl.pallas_call(
        prepare_kernel,
        out_shape=(
            jax.ShapeDtypeStruct((parts, neighbours + 8, width), jnp.int16),
            jax.ShapeDtypeStruct((parts * WORDS // 128, 128), jnp.int32),
        ),
        scratch_shapes=[
            pltpu.VMEM((neighbours, width), jnp.int32),
            pltpu.VMEM((neighbours, width), jnp.int32),
            pltpu.VMEM((parts * cap // 128, 128), jnp.int32),
        ],
        name="prepare",
        compiler_params=pltpu.CompilerParams(vmem_limit_bytes=16 * 2**20),
    )(slots, count, own, fetch)


def exchange_kernel(
    slab_ref, words_ref, slab_out, words_out, slab_send, slab_recv, words_send, words_recv, own_sem
):
    n, q = lax.axis_index("neg"), lax.axis_index("qry")
    x, y = n // SIDE, n % SIDE
    lines = WORDS // 128
    last = len(HOPS) - 1

    def target(k):
        dx, dy = HOPS[k][0]
        return lax.rem(x + SIDE - dx, SIDE) * SIDE + lax.rem(y + SIDE - dy, SIDE)

    barrier = pltpu.get_barrier_semaphore()
    for k in range(last):
        pl.semaphore_signal(barrier, inc=1, device_id=(target(k), q), device_id_type=MESH)
    pl.semaphore_wait(barrier, last)

    copies = []
    for k in range(last):
        to = target(k)
        for source, out, send, recv, at in (
            (slab_ref.at[to], slab_out.at[k], slab_send, slab_recv, None),
            (
                words_ref.at[pl.ds(to * lines, lines)], words_out.at[pl.ds(k * lines, lines)],
                words_send, words_recv, None,
            ),
        ):
            copies.append(
                pltpu.make_async_remote_copy(
                    src_ref=source, dst_ref=out, send_sem=send.at[k], recv_sem=recv.at[k],
                    device_id=(to, q), device_id_type=MESH,
                )
            )
            copies[-1].start()
    own = [
        pltpu.make_async_copy(slab_ref.at[n], slab_out.at[last], own_sem.at[0]),
        pltpu.make_async_copy(
            words_ref.at[pl.ds(n * lines, lines)], words_out.at[pl.ds(last * lines, lines)],
            own_sem.at[1],
        ),
    ]
    for copy in own:
        copy.start()
    for copy in own:
        copy.wait()
    for copy in copies:
        copy.wait_recv()
    for copy in copies:
        copy.wait_send()


def exchange(slab, words):
    vmem = pl.BlockSpec(memory_space=pltpu.VMEM)
    dma = pltpu.SemaphoreType.DMA
    hops = len(HOPS) - 1
    return pl.pallas_call(
        exchange_kernel,
        in_specs=[vmem, vmem],
        out_specs=(vmem, vmem),
        out_shape=(
            jax.ShapeDtypeStruct(slab.shape, slab.dtype),
            jax.ShapeDtypeStruct(words.shape, words.dtype),
        ),
        scratch_shapes=[dma((hops,)), dma((hops,)), dma((hops,)), dma((hops,)), dma((2,))],
        name="exchange",
        compiler_params=pltpu.CompilerParams(
            collective_id=1, has_side_effects=True, vmem_limit_bytes=8 * 2**20
        ),
    )(slab, words)


def counts_kernel(words_ref, slab_ref, out_ref):
    cap, count = out_ref.shape[1:]
    neighbours = slab_ref.shape[1] - 8
    tile = 16
    row = lax.broadcasted_iota(jnp.int32, (tile, 128), 0).astype(jnp.int16)
    zero = jnp.zeros((tile, 128), jnp.bfloat16)

    def build(t, _):
        lanes = pl.ds(pl.multiple_of(t * 128, 128), 128)
        rows = slab_ref[0, :, lanes].astype(jnp.int32)
        most = words_ref[pl.program_id(0) * WORDS + cap + count + t]
        scale = 1.0 / rows[neighbours + 1 : neighbours + 2].astype(jnp.float32)
        scale = jnp.broadcast_to(scale, (tile, 128)).astype(jnp.bfloat16)

        def spread(k):
            return jnp.broadcast_to(rows[k : k + 1], (tile, 128)).astype(jnp.int16)

        slots = [spread(k) for k in range(6)]
        for i in range(cap // tile):
            here = row + jnp.int16(i * tile)
            total = jnp.where(slots[0] == here, scale, zero)
            for slot in slots[1:]:
                total = total + jnp.where(slot == here, scale, zero)
            out_ref[0, i * tile : (i + 1) * tile, lanes] = total

        def more(first, step):
            if first >= neighbours:
                return

            @pl.when(most > first)
            def _():
                last = min(first + step, neighbours)
                slots = [spread(k) for k in range(first, last)]

                def body(i, _):
                    at = pl.ds(pl.multiple_of(i * tile, tile), tile)
                    here = row + (i * tile).astype(jnp.int16)
                    total = out_ref[0, at, lanes]
                    for slot in slots:
                        total = total + jnp.where(slot == here, scale, zero)
                    out_ref[0, at, lanes] = total
                    return 0

                lax.fori_loop(0, cap // tile, body, 0, unroll=first < 8)
                more(last, 2 * step)

        more(6, 2)
        return 0

    lax.fori_loop(0, count // 128, build, 0)


def counts_blocks(words, slab, cap):
    parts, rows, count = slab.shape
    return pl.pallas_call(
        counts_kernel,
        grid=(parts,),
        in_specs=[
            pl.BlockSpec(memory_space=pltpu.SMEM),
            pl.BlockSpec((1, rows, count), lambda i: (i, 0, 0)),
        ],
        out_specs=pl.BlockSpec((1, cap, count), lambda i: (i, 0, 0)),
        out_shape=pltpu.HBM((parts, cap, count), jnp.bfloat16),
        name="counts",
        cost_estimate=pl.CostEstimate(
            flops=10**9, bytes_accessed=12 * 2**20, transcendentals=0
        ),
        compiler_params=pltpu.CompilerParams(vmem_limit_bytes=6 * 2**20),
    )(words, slab)


def join(peak, total, other_peak, other_total):
    top = jnp.maximum(peak, other_peak)
    return top, total * jnp.exp(peak - top) + other_total * jnp.exp(other_peak - top)


def tower_kernel(
    parts, qrys, words_ref, counts_ref, items_ref, mw_ref, mb_ref, nw_ref,
    sw_ref, bias_ref, log_ref, queries_ref, negative_ref, lse_ref, gathered,
    u_ref, v_ref, items_tile, landed, summed, matrix, g_ref, z_ref, column_ref, partial, first_in,
    second_out, second_in, items_sem, matrix_sem, tile_sem, block_send, block_recv, query_send,
    query_recv, first_send, first_recv, second_send, second_recv,
):
    n, q = lax.axis_index("neg"), lax.axis_index("qry")
    x, y = n // SIDE, n % SIDE
    z, core = q // 2, q % 2
    cap, count = counts_ref.shape[1:]
    own_rows = queries_ref.shape[0]
    half = count // 2

    def matrix_load(k):
        slot = lax.rem(k, 2)
        return pltpu.make_async_copy(counts_ref.at[k], matrix.at[slot], matrix_sem.at[slot])

    matrix_load(0).start()
    item_rows = items_tile.shape[1]
    item_tiles = items_ref.shape[0] // item_rows

    def items_load(t):
        slot = lax.rem(t, 2)
        return pltpu.make_async_copy(
            items_ref.at[pl.ds(t * item_rows, item_rows)], items_tile.at[slot], items_sem.at[slot]
        )

    items_load(0).start()
    barrier = pltpu.get_barrier_semaphore()
    for i in range(1, qrys):
        pl.semaphore_signal(
            barrier, inc=1, device_id=(n, lax.rem(q + i, qrys)), device_id_type=MESH
        )
    for i in range(1, parts):
        pl.semaphore_signal(
            barrier, inc=1, device_id=(lax.rem(n + i, parts), q), device_id_type=MESH
        )
    pl.semaphore_wait(barrier, qrys + parts - 2)

    def hop(k, h):
        axis, step = HOPS[k][1]
        if axis == 0:
            to = lax.rem(x + step + SIDE, SIDE) * SIDE + y
        else:
            to = x * SIDE + lax.rem(y + step + SIDE, SIDE)
        rows = pl.ds(h * half, half)
        source = summed.at[k, rows]
        return pltpu.make_async_remote_copy(
            src_ref=source, dst_ref=landed.at[k, rows],
            send_sem=block_send.at[k, h], recv_sem=block_recv.at[k, h],
            device_id=(to, q), device_id_type=MESH,
        )

    up = (n, lax.rem(z + 1, qrys // 2) * 2 + core)
    down = (n, lax.rem(z + qrys // 2 - 1, qrys // 2) * 2 + core)
    partner = (n, z * 2 + 1 - core)
    below, above = down[1], up[1]
    across = lax.rem(z + 2, qrys // 2) * 2 + core

    def spread(k, block, part, to, source=None):
        rows = pl.ds(0, own_rows) if part is None else pl.ds(part * (own_rows // 2), own_rows // 2)
        return pltpu.make_async_remote_copy(
            src_ref=gathered.at[block, rows] if source is None else source,
            dst_ref=gathered.at[block, rows],
            send_sem=query_send.at[k], recv_sem=query_recv.at[k],
            device_id=to, device_id_type=MESH,
        )

    spreads = [
        spread(0, q, None, up, queries_ref),
        spread(1, q, None, down, queries_ref),
        spread(2, q, None, partner, queries_ref),
        spread(3, below, 0, up),
        spread(4, above, 1, down),
        spread(5, below, None, partner),
        spread(6, above, None, partner),
        spread(7, across, 0, partner),
        spread(8, across, 1, partner),
    ]

    hops = {(k, h): hop(k, h) for k in range(len(HOPS) - 1) for h in range(2)}
    for k in range(3):
        spreads[k].start()
    own_log = jnp.log(log_ref[pl.ds(q, 1), :].astype(jnp.float32))
    wide = jnp.broadcast_to(own_log, (8, count))
    column_ref[...] = jnp.transpose(wide)[:, 0:1]

    step = 64

    def table(t, _):
        items_load(t).wait()

        @pl.when(t + 1 < item_tiles)
        def _():
            items_load(t + 1).start()

        rows = items_tile[lax.rem(t, 2)]
        message = jnp.dot(rows, mw_ref[...], preferred_element_type=jnp.float32) + mb_ref[...]
        message = jnp.maximum(message, 0.0).astype(jnp.bfloat16)
        u = jnp.dot(message, nw_ref[...], preferred_element_type=jnp.float32)
        v = jnp.dot(rows, sw_ref[...], preferred_element_type=jnp.float32)
        for j in range(4):
            cols = slice(128 * j, 128 * j + 128)
            u_ref[pl.ds(t * item_rows * 4 + j, item_rows, stride=4), :] = u[:, cols]
            v_ref[pl.ds(t * item_rows * 4 + j, item_rows, stride=4), :] = v[:, cols]
        return 0

    v_ref[pl.ds(4 * items_ref.shape[0], 8), :] = jnp.zeros((8, 128), jnp.float32)
    lax.fori_loop(0, item_tiles, table, 0)
    unroll = 32
    u_rows = u_ref.reshape(u_ref.shape[0] // 4, 4, 128)
    v_rows = v_ref.reshape(v_ref.shape[0] // 4, 4, 128)

    def compute(k):
        def fetch(t, _):
            base = k * WORDS + t * unroll
            for s in range(unroll):
                g_ref[pl.ds(pl.multiple_of((t * unroll + s) * 4, 4), 4), :] = u_rows[words_ref[base + s]]
            return 0

        def own(t, _):
            own_base = k * WORDS + cap + t * unroll
            for s in range(unroll):
                z_ref[pl.ds(pl.multiple_of((t * unroll + s) * 4, 4), 4), :] = v_rows[words_ref[own_base + s]]
            return 0

        lax.fori_loop(0, cap // unroll, fetch, 0)
        lax.fori_loop(0, count // unroll, own, 0)
        matrix_load(k).wait()

        @pl.when(k + 1 < len(HOPS))
        def _():
            matrix_load(k + 1).start()

        rows = jnp.concatenate(
            [g_ref[pl.ds(j, cap, stride=4), :].astype(jnp.bfloat16) for j in range(4)], axis=1
        )
        for h in range(2):
            at = slice(h * half, h * half + half)
            mean = lax.dot_general(
                matrix[lax.rem(k, 2), :, at], rows, (((0,), (0,)), ((), ())),
                preferred_element_type=jnp.float32,
            )
            for j in range(4):
                cols = slice(128 * j, 128 * j + 128)
                own_part = z_ref[pl.ds(h * half * 4 + j, half, stride=4), :]
                summed[k, at, cols] = (mean[:, cols] + own_part).astype(jnp.bfloat16)

    def form(k, h):
        for child in CHILDREN[k]:
            hops[child, h].wait_recv()

        def body(t, _):
            rows = pl.ds(pl.multiple_of(h * half + t * step, step), step)
            total = summed[k, rows, :].astype(jnp.float32)
            for child in CHILDREN[k]:
                total = total + landed[child, rows, :].astype(jnp.float32)
            if HOPS[k][1] is None:
                hidden = jnp.maximum(total + bias_ref[...], 0.0)
                mean = jnp.mean(hidden * hidden, axis=-1, keepdims=True)
                negative_ref[rows, :] = (hidden * lax.rsqrt(mean + 0.25)).astype(jnp.bfloat16)
            else:
                summed[k, rows, :] = total.astype(jnp.bfloat16)
            return 0

        lax.fori_loop(0, half // step, body, 0)

    def after(k):
        if k == NEAR:
            spreads[0].wait_recv()
            spreads[3].start()
            spreads[5].start()
            spreads[1].wait_recv()
            spreads[4].start()
            spreads[6].start()
        if k == FAR:
            spreads[3].wait_recv()
            spreads[7].start()
            spreads[4].wait_recv()
            spreads[8].start()
        for h in range(2):
            if CHILDREN[k]:
                form(k, h)
            if HOPS[k][1] is not None:
                hops[k, h].start()

    def block(k, _):
        compute(k)
        for i in range(len(HOPS)):
            pl.when(k == i)(functools.partial(after, i))
        return 0

    lax.fori_loop(0, len(HOPS), block, 0)
    for k in (2, 5, 6, 7, 8):
        spreads[k].wait_recv()

    tile = own_rows // 2

    def score(block, h):
        cols = slice(h * tile, h * tile + tile)
        scores = lax.dot_general(
            negative_ref[...], matrix[h, 0:tile, :], (((1,), (1,)), ((), ())),
            preferred_element_type=jnp.float32,
        )
        scores = 0.25 * scores - column_ref[...]
        peak = jnp.max(scores, axis=0, keepdims=True)
        partial[block, 0:1, cols] = peak
        partial[block, 1:2, cols] = jnp.sum(jnp.exp(scores - peak), axis=0, keepdims=True)

    def tile_load(i, h):
        rows = pl.ds(h * tile, tile)
        source = queries_ref.at[rows] if i is None else gathered.at[lax.rem(q + i, qrys), rows]
        return pltpu.make_async_copy(source, matrix.at[h, pl.ds(0, tile)], tile_sem.at[h])

    def tile_start(i, h):
        @pl.when(i < qrys)
        def _():
            tile_load(i, h).start()

        @pl.when(i == qrys)
        def _():
            tile_load(None, h).start()

    for h in range(2):
        tile_load(1, h).start()

    def first(i):
        to = lax.rem(q + i, qrys)
        return pltpu.make_async_remote_copy(
            src_ref=partial.at[to], dst_ref=first_in.at[i],
            send_sem=first_send.at[i], recv_sem=first_recv.at[i],
            device_id=(n, to), device_id_type=MESH,
        )

    def each(i, _):
        for h in range(2):
            tile_load(None, h).wait()
            score(lax.rem(q + i, qrys), h)
            tile_start(i + 1, h)

        @pl.when(i > 1)
        def _():
            first(i - 1).start()

        return 0

    lax.fori_loop(1, qrys + 1, each, 0)
    peak, total = partial[q, 0:1, :], partial[q, 1:2, :]
    for i in range(1, qrys):
        first(i).wait_recv()
        peak, total = join(peak, total, first_in[i, 0:1, :], first_in[i, 1:2, :])
    second_out[0:1, :] = peak
    second_out[1:2, :] = total

    def second(i):
        return pltpu.make_async_remote_copy(
            src_ref=second_out, dst_ref=second_in.at[i],
            send_sem=second_send.at[i], recv_sem=second_recv.at[i],
            device_id=(lax.rem(n + i, parts), q), device_id_type=MESH,
        )

    for i in range(1, parts):
        second(i).start()
    for k in range(len(HOPS) - 1):
        for h in range(2):
            hops[k, h].wait_send()
    for k in range(9):
        spreads[k].wait_send()
    for i in range(1, qrys):
        first(i).wait_send()
    for i in range(1, parts):
        second(i).wait_recv()
        peak, total = join(peak, total, second_in[i, 0:1, :], second_in[i, 1:2, :])
    lse_ref[...] = peak + jnp.log(total) - math.log(count * parts * qrys)
    for i in range(1, parts):
        second(i).wait_send()


def tower(words, counts, items, weights, bias, log_count, queries, qrys):
    parts, cap, count = counts.shape
    own_rows, width = queries.shape
    vmem = pl.BlockSpec(memory_space=pltpu.VMEM)
    smem = pl.BlockSpec(memory_space=pltpu.SMEM)
    hbm = pl.BlockSpec(memory_space=pltpu.HBM)
    dma = pltpu.SemaphoreType.DMA
    hops = len(HOPS) - 1
    return pl.pallas_call(
        functools.partial(tower_kernel, parts, qrys),
        in_specs=[smem, hbm, hbm, vmem, vmem, vmem, vmem, vmem, vmem, hbm],
        out_specs=(vmem, vmem, hbm),
        out_shape=(
            pltpu.VMEM((count, width), jnp.bfloat16),
            pltpu.VMEM((1, own_rows), jnp.float32),
            jax.ShapeDtypeStruct((qrys, own_rows, width), jnp.bfloat16),
        ),
        scratch_shapes=[
            pltpu.VMEM((4 * items.shape[0], 128), jnp.float32),
            pltpu.VMEM((4 * items.shape[0] + 8, 128), jnp.float32),
            pltpu.VMEM((2, 512, width), jnp.bfloat16),
            pltpu.VMEM((hops, count, width), jnp.bfloat16),
            pltpu.VMEM((hops + 1, count, width), jnp.bfloat16),
            pltpu.VMEM((2, cap, count), jnp.bfloat16),
            pltpu.VMEM((4 * cap, 128), jnp.float32),
            pltpu.VMEM((4 * count, 128), jnp.float32),
            pltpu.VMEM((count, 1), jnp.float32),
            pltpu.VMEM((qrys, 2, own_rows), jnp.float32),
            pltpu.VMEM((qrys, 2, own_rows), jnp.float32),
            pltpu.VMEM((2, own_rows), jnp.float32),
            pltpu.VMEM((parts, 2, own_rows), jnp.float32),
            dma((2,)), dma((2,)), dma((2,)), dma((hops, 2)), dma((hops, 2)), dma((9,)), dma((9,)),
            dma((qrys,)), dma((qrys,)), dma((parts,)), dma((parts,)),
        ],
        name="tower",
        compiler_params=pltpu.CompilerParams(
            collective_id=0, has_side_effects=True, vmem_limit_bytes=TOWER_VMEM
        ),
    )(words, counts, items, *weights, bias, log_count, queries)


def per_device(
    items_table,
    fetch_rows,
    neighbour_slots,
    neighbour_count,
    self_slot,
    negative_count,
    message_weight,
    message_bias,
    self_weight,
    neighbour_weight,
    output_bias,
    queries,
):
    parts, cap = fetch_rows.shape
    count, neighbours = neighbour_slots.shape

    assert items_table.shape[0] == ITEM_ROWS
    lists = [
        pltpu.with_memory_space_constraint(x, pltpu.HBM)
        for x in (neighbour_slots.T, neighbour_count[None], self_slot[None], fetch_rows)
    ]
    slab, words = prepare(*lists)
    slab, words = exchange(slab, words)
    words = words.reshape(-1)

    matrices = counts_blocks(words, slab, cap)
    matrices = pltpu.with_memory_space_constraint(matrices, pltpu.HBM)
    negative_embed, query_lse, _ = tower(
        words, matrices, items_table,
        (message_weight, message_bias[None], neighbour_weight, self_weight),
        output_bias[None], negative_count.reshape(-1, count), queries,
        lax.axis_size("qry"),
    )
    return (negative_embed, query_lse[0])


def solution(mesh):
    in_specs = (
        P("neg", None),
        P(("neg", "qry"), None),
        P(("neg", "qry"), None),
        P(("neg", "qry")),
        P(("neg", "qry")),
        P("neg"),
        P(),
        P(),
        P(),
        P(),
        P(),
        P("qry", None),
    )
    out_specs = (P(("neg", "qry"), None), P("qry"))
    return jax.shard_map(
        per_device, mesh=mesh, in_specs=in_specs, out_specs=out_specs, check_vma=False
    )
```

```python
import functools
import math

import jax
import jax.numpy as jnp
from jax import lax
from jax.experimental import pallas as pl
from jax.experimental.pallas import tpu as pltpu
from jax.sharding import PartitionSpec as P


SIDE = 4
HOPS = (
    ((2, 2), (0, 1)),
    ((2, 1), (0, -1)),
    ((3, 2), (1, 1)),
    ((2, 0), (0, 1)),
    ((1, 2), (1, -1)),
    ((2, 3), (0, -1)),
    ((0, 2), (1, 1)),
    ((1, 1), (0, 1)),
    ((3, 1), (1, 1)),
    ((1, 3), (1, -1)),
    ((3, 3), (0, -1)),
    ((1, 0), (0, 1)),
    ((0, 1), (1, 1)),
    ((0, 3), (1, -1)),
    ((3, 0), (0, -1)),
    ((0, 0), None),
)
PLACE = {offset: k for k, (offset, _) in enumerate(HOPS)}
CHILDREN = [[] for _ in HOPS]
for _k, ((_dx, _dy), _way) in enumerate(HOPS):
    if _way is not None:
        _to = ((_dx - _way[1]) % SIDE, _dy) if _way[0] == 0 else (_dx, (_dy - _way[1]) % SIDE)
        CHILDREN[PLACE[_to]].append(_k)
NEAR, FAR = 4, 10
TOWER_VMEM = 60 * 2**20
WORDS = 2048
ITEM_ROWS = 8192
MESH = pl.DeviceIdType.MESH


def prepare_kernel(
    slots_ref, count_ref, self_ref, fetch_ref, slab_ref, words_ref, owner_ref, local_ref, table_ref
):
    neighbours, width = slots_ref.shape
    parts, cap = fetch_ref.shape

    slots = slots_ref[...]
    owner = ((slots.astype(jnp.float32) + 0.5) * (1.0 / cap)).astype(jnp.int32)
    order = lax.broadcasted_iota(jnp.int32, (neighbours, width), 0)
    local_ref[...] = slots - owner * cap
    owner_ref[...] = jnp.where(order < count_ref[...], owner, -1)

    for i in range(cap // 128):
        rows = fetch_ref[:, 128 * i : 128 * i + 128]
        table_ref[pl.ds(i, parts, stride=cap // 128), :] = rows
        words_ref[pl.ds(i, parts, stride=WORDS // 128), :] = rows
    chunks = parts * cap // 128
    own = self_ref[...]
    high = lax.shift_right_logical(own, 7)
    low = own - lax.shift_left(high, 7)
    pick = (lax.broadcasted_iota(jnp.int32, (chunks, width), 0) == high).astype(jnp.float32)
    pick = pick.astype(jnp.bfloat16)
    rows = table_ref[...]
    upper = lax.shift_right_logical(rows, 7)
    lower = rows - lax.shift_left(upper, 7)
    found = [
        lax.dot_general(
            part.astype(jnp.float32).astype(jnp.bfloat16), pick, (((0,), (0,)), ((), ())),
            preferred_element_type=jnp.float32,
        )
        for part in (upper, lower)
    ]
    at = lax.broadcasted_iota(jnp.int32, (128, width), 0) == low
    own_row = jnp.sum(jnp.where(at, 128.0 * found[0] + found[1], 0.0), axis=0, keepdims=True)
    own_owner = ((own.astype(jnp.float32) + 0.5) * (1.0 / cap)).astype(jnp.int32)
    mine = lax.broadcasted_iota(jnp.int32, (parts, width), 0) == own_owner
    own_rows = jnp.where(mine, own_row.astype(jnp.int32), ITEM_ROWS)
    for i in range(width // 128):
        words_ref[pl.ds(cap // 128 + i, parts, stride=WORDS // 128), :] = own_rows[
            :, 128 * i : 128 * i + 128
        ]
    slab_ref[:, neighbours:, :] = jnp.broadcast_to(
        count_ref[...][None], (parts, slab_ref.shape[1] - neighbours, width)
    ).astype(jnp.int16)

    part = lax.broadcasted_iota(jnp.int32, (parts, 128), 0).astype(jnp.int16)
    one = jnp.ones((parts, 128), jnp.int16)
    zero = jnp.zeros((parts, 128), jnp.int16)
    lane = lax.broadcasted_iota(jnp.int32, (parts, 128), 1)
    most = jnp.zeros((parts, 128), jnp.int32)
    for t in range(width // 128):
        lanes = slice(128 * t, 128 * t + 128)
        seen = zero
        found = [zero - one] * neighbours
        for k in range(neighbours):
            owner = jnp.broadcast_to(owner_ref[k : k + 1, lanes], (parts, 128)).astype(jnp.int16)
            local = jnp.broadcast_to(local_ref[k : k + 1, lanes], (parts, 128)).astype(jnp.int16)
            mine = owner == part
            rank = jnp.where(mine, seen, zero - one)
            for j in range(k + 1):
                found[j] = jnp.where(rank == jnp.int16(j), local, found[j])
            seen = seen + jnp.where(mine, one, zero)
        for j in range(neighbours):
            slab_ref[:, j, lanes] = found[j]
        peak = jnp.max(seen.astype(jnp.int32), axis=1, keepdims=True)
        most = jnp.where(lane == t, peak, most)
    words_ref[pl.ds((cap + width) // 128, parts, stride=WORDS // 128), :] = most


def prepare(slots, count, own, fetch):
    neighbours, width = slots.shape
    parts, cap = fetch.shape
    return pl.pallas_call(
        prepare_kernel,
        out_shape=(
            jax.ShapeDtypeStruct((parts, neighbours + 8, width), jnp.int16),
            jax.ShapeDtypeStruct((parts * WORDS // 128, 128), jnp.int32),
        ),
        scratch_shapes=[
            pltpu.VMEM((neighbours, width), jnp.int32),
            pltpu.VMEM((neighbours, width), jnp.int32),
            pltpu.VMEM((parts * cap // 128, 128), jnp.int32),
        ],
        name="prepare",
        compiler_params=pltpu.CompilerParams(vmem_limit_bytes=16 * 2**20),
    )(slots, count, own, fetch)


def exchange_kernel(
    slab_ref, words_ref, slab_out, words_out, slab_send, slab_recv, words_send, words_recv, own_sem
):
    n, q = lax.axis_index("neg"), lax.axis_index("qry")
    x, y = n // SIDE, n % SIDE
    lines = WORDS // 128
    last = len(HOPS) - 1

    def target(k):
        dx, dy = HOPS[k][0]
        return lax.rem(x + SIDE - dx, SIDE) * SIDE + lax.rem(y + SIDE - dy, SIDE)

    barrier = pltpu.get_barrier_semaphore()
    for k in range(last):
        pl.semaphore_signal(barrier, inc=1, device_id=(target(k), q), device_id_type=MESH)
    pl.semaphore_wait(barrier, last)

    copies = []
    for k in range(last):
        to = target(k)
        for source, out, send, recv, at in (
            (slab_ref.at[to], slab_out.at[k], slab_send, slab_recv, None),
            (
                words_ref.at[pl.ds(to * lines, lines)], words_out.at[pl.ds(k * lines, lines)],
                words_send, words_recv, None,
            ),
        ):
            copies.append(
                pltpu.make_async_remote_copy(
                    src_ref=source, dst_ref=out, send_sem=send.at[k], recv_sem=recv.at[k],
                    device_id=(to, q), device_id_type=MESH,
                )
            )
            copies[-1].start()
    own = [
        pltpu.make_async_copy(slab_ref.at[n], slab_out.at[last], own_sem.at[0]),
        pltpu.make_async_copy(
            words_ref.at[pl.ds(n * lines, lines)], words_out.at[pl.ds(last * lines, lines)],
            own_sem.at[1],
        ),
    ]
    for copy in own:
        copy.start()
    for copy in own:
        copy.wait()
    for copy in copies:
        copy.wait_recv()
    for copy in copies:
        copy.wait_send()


def exchange(slab, words):
    vmem = pl.BlockSpec(memory_space=pltpu.VMEM)
    dma = pltpu.SemaphoreType.DMA
    hops = len(HOPS) - 1
    return pl.pallas_call(
        exchange_kernel,
        in_specs=[vmem, vmem],
        out_specs=(vmem, vmem),
        out_shape=(
            jax.ShapeDtypeStruct(slab.shape, slab.dtype),
            jax.ShapeDtypeStruct(words.shape, words.dtype),
        ),
        scratch_shapes=[dma((hops,)), dma((hops,)), dma((hops,)), dma((hops,)), dma((2,))],
        name="exchange",
        compiler_params=pltpu.CompilerParams(
            collective_id=1, has_side_effects=True, vmem_limit_bytes=8 * 2**20
        ),
    )(slab, words)


def counts_kernel(words_ref, slab_ref, out_ref):
    cap, count = out_ref.shape[1:]
    neighbours = slab_ref.shape[1] - 8
    tile = 16
    row = lax.broadcasted_iota(jnp.int32, (tile, 128), 0).astype(jnp.int16)
    zero = jnp.zeros((tile, 128), jnp.bfloat16)

    def build(t, _):
        lanes = pl.ds(pl.multiple_of(t * 128, 128), 128)
        rows = slab_ref[0, :, lanes].astype(jnp.int32)
        most = words_ref[pl.program_id(0) * WORDS + cap + count + t]
        scale = 1.0 / rows[neighbours + 1 : neighbours + 2].astype(jnp.float32)
        scale = jnp.broadcast_to(scale, (tile, 128)).astype(jnp.bfloat16)

        def spread(k):
            return jnp.broadcast_to(rows[k : k + 1], (tile, 128)).astype(jnp.int16)

        slots = [spread(k) for k in range(6)]
        for i in range(cap // tile):
            here = row + jnp.int16(i * tile)
            total = jnp.where(slots[0] == here, scale, zero)
            for slot in slots[1:]:
                total = total + jnp.where(slot == here, scale, zero)
            out_ref[0, i * tile : (i + 1) * tile, lanes] = total

        def more(first, step):
            if first >= neighbours:
                return

            @pl.when(most > first)
            def _():
                last = min(first + step, neighbours)
                slots = [spread(k) for k in range(first, last)]

                def body(i, _):
                    at = pl.ds(pl.multiple_of(i * tile, tile), tile)
                    here = row + (i * tile).astype(jnp.int16)
                    total = out_ref[0, at, lanes]
                    for slot in slots:
                        total = total + jnp.where(slot == here, scale, zero)
                    out_ref[0, at, lanes] = total
                    return 0

                lax.fori_loop(0, cap // tile, body, 0, unroll=first < 8)
                more(last, 2 * step)

        more(6, 2)
        return 0

    lax.fori_loop(0, count // 128, build, 0)


def counts_blocks(words, slab, cap):
    parts, rows, count = slab.shape
    return pl.pallas_call(
        counts_kernel,
        grid=(parts,),
        in_specs=[
            pl.BlockSpec(memory_space=pltpu.SMEM),
            pl.BlockSpec((1, rows, count), lambda i: (i, 0, 0)),
        ],
        out_specs=pl.BlockSpec((1, cap, count), lambda i: (i, 0, 0)),
        out_shape=pltpu.HBM((parts, cap, count), jnp.bfloat16),
        name="counts",
        cost_estimate=pl.CostEstimate(
            flops=10**9, bytes_accessed=12 * 2**20, transcendentals=0
        ),
        compiler_params=pltpu.CompilerParams(vmem_limit_bytes=6 * 2**20),
    )(words, slab)


def join(peak, total, other_peak, other_total):
    top = jnp.maximum(peak, other_peak)
    return top, total * jnp.exp(peak - top) + other_total * jnp.exp(other_peak - top)


def tower_kernel(
    parts, qrys, words_ref, counts_ref, items_ref, mw_ref, mb_ref, nw_ref,
    sw_ref, bias_ref, log_ref, queries_ref, negative_ref, lse_ref, gathered,
    u_ref, v_ref, items_tile, landed, summed, matrix, g_ref, z_ref, column_ref, partial, first_in,
    second_out, second_in, items_sem, matrix_sem, tile_sem, block_send, block_recv, query_send,
    query_recv, first_send, first_recv, second_send, second_recv,
):
    n, q = lax.axis_index("neg"), lax.axis_index("qry")
    x, y = n // SIDE, n % SIDE
    z, core = q // 2, q % 2
    cap, count = counts_ref.shape[1:]
    own_rows = queries_ref.shape[0]
    half = count // 2

    def matrix_load(k):
        slot = lax.rem(k, 2)
        return pltpu.make_async_copy(counts_ref.at[k], matrix.at[slot], matrix_sem.at[slot])

    matrix_load(0).start()
    item_rows = items_tile.shape[1]
    item_tiles = items_ref.shape[0] // item_rows

    def items_load(t):
        slot = lax.rem(t, 2)
        return pltpu.make_async_copy(
            items_ref.at[pl.ds(t * item_rows, item_rows)], items_tile.at[slot], items_sem.at[slot]
        )

    items_load(0).start()
    barrier = pltpu.get_barrier_semaphore()
    for i in range(1, qrys):
        pl.semaphore_signal(
            barrier, inc=1, device_id=(n, lax.rem(q + i, qrys)), device_id_type=MESH
        )
    for i in range(1, parts):
        pl.semaphore_signal(
            barrier, inc=1, device_id=(lax.rem(n + i, parts), q), device_id_type=MESH
        )
    pl.semaphore_wait(barrier, qrys + parts - 2)

    def hop(k, h):
        axis, step = HOPS[k][1]
        if axis == 0:
            to = lax.rem(x + step + SIDE, SIDE) * SIDE + y
        else:
            to = x * SIDE + lax.rem(y + step + SIDE, SIDE)
        rows = pl.ds(h * half, half)
        source = summed.at[k, rows]
        return pltpu.make_async_remote_copy(
            src_ref=source, dst_ref=landed.at[k, rows],
            send_sem=block_send.at[k, h], recv_sem=block_recv.at[k, h],
            device_id=(to, q), device_id_type=MESH,
        )

    up = (n, lax.rem(z + 1, qrys // 2) * 2 + core)
    down = (n, lax.rem(z + qrys // 2 - 1, qrys // 2) * 2 + core)
    partner = (n, z * 2 + 1 - core)
    below, above = down[1], up[1]
    across = lax.rem(z + 2, qrys // 2) * 2 + core

    def spread(k, block, part, to, source=None):
        rows = pl.ds(0, own_rows) if part is None else pl.ds(part * (own_rows // 2), own_rows // 2)
        return pltpu.make_async_remote_copy(
            src_ref=gathered.at[block, rows] if source is None else source,
            dst_ref=gathered.at[block, rows],
            send_sem=query_send.at[k], recv_sem=query_recv.at[k],
            device_id=to, device_id_type=MESH,
        )

    spreads = [
        spread(0, q, None, up, queries_ref),
        spread(1, q, None, down, queries_ref),
        spread(2, q, None, partner, queries_ref),
        spread(3, below, 0, up),
        spread(4, above, 1, down),
        spread(5, below, None, partner),
        spread(6, above, None, partner),
        spread(7, across, 0, partner),
        spread(8, across, 1, partner),
    ]

    hops = {(k, h): hop(k, h) for k in range(len(HOPS) - 1) for h in range(2)}
    for k in range(3):
        spreads[k].start()
    own_log = jnp.log(log_ref[pl.ds(q, 1), :].astype(jnp.float32))
    wide = jnp.broadcast_to(own_log, (8, count))
    column_ref[...] = jnp.transpose(wide)[:, 0:1]

    step = 64

    def table(t, _):
        items_load(t).wait()

        @pl.when(t + 1 < item_tiles)
        def _():
            items_load(t + 1).start()

        rows = items_tile[lax.rem(t, 2)]
        message = jnp.dot(rows, mw_ref[...], preferred_element_type=jnp.float32) + mb_ref[...]
        message = jnp.maximum(message, 0.0).astype(jnp.bfloat16)
        u = jnp.dot(message, nw_ref[...], preferred_element_type=jnp.float32)
        v = jnp.dot(rows, sw_ref[...], preferred_element_type=jnp.float32)
        for j in range(4):
            cols = slice(128 * j, 128 * j + 128)
            u_ref[pl.ds(t * item_rows * 4 + j, item_rows, stride=4), :] = u[:, cols]
            v_ref[pl.ds(t * item_rows * 4 + j, item_rows, stride=4), :] = v[:, cols]
        return 0

    v_ref[pl.ds(4 * items_ref.shape[0], 8), :] = jnp.zeros((8, 128), jnp.float32)
    lax.fori_loop(0, item_tiles, table, 0)
    unroll = 64
    u_rows = u_ref.reshape(u_ref.shape[0] // 4, 4, 128)
    v_rows = v_ref.reshape(v_ref.shape[0] // 4, 4, 128)

    def compute(k):
        def fetch(t, _):
            base = k * WORDS + t * unroll
            for s in range(unroll):
                g_ref[pl.ds(pl.multiple_of((t * unroll + s) * 4, 4), 4), :] = u_rows[words_ref[base + s]]
            return 0

        def own(t, _):
            own_base = k * WORDS + cap + t * unroll
            for s in range(unroll):
                z_ref[pl.ds(pl.multiple_of((t * unroll + s) * 4, 4), 4), :] = v_rows[words_ref[own_base + s]]
            return 0

        lax.fori_loop(0, cap // unroll, fetch, 0)
        lax.fori_loop(0, count // unroll, own, 0)
        matrix_load(k).wait()

        @pl.when(k + 1 < len(HOPS))
        def _():
            matrix_load(k + 1).start()

        rows = jnp.concatenate(
            [g_ref[pl.ds(j, cap, stride=4), :].astype(jnp.bfloat16) for j in range(4)], axis=1
        )
        for h in range(2):
            at = slice(h * half, h * half + half)
            mean = lax.dot_general(
                matrix[lax.rem(k, 2), :, at], rows, (((0,), (0,)), ((), ())),
                preferred_element_type=jnp.float32,
            )
            for j in range(4):
                cols = slice(128 * j, 128 * j + 128)
                own_part = z_ref[pl.ds(h * half * 4 + j, half, stride=4), :]
                summed[k, at, cols] = (mean[:, cols] + own_part).astype(jnp.bfloat16)

    def form(k, h):
        for child in CHILDREN[k]:
            hops[child, h].wait_recv()

        def body(t, _):
            rows = pl.ds(pl.multiple_of(h * half + t * step, step), step)
            total = summed[k, rows, :].astype(jnp.float32)
            for child in CHILDREN[k]:
                total = total + landed[child, rows, :].astype(jnp.float32)
            if HOPS[k][1] is None:
                hidden = jnp.maximum(total + bias_ref[...], 0.0)
                mean = jnp.mean(hidden * hidden, axis=-1, keepdims=True)
                negative_ref[rows, :] = (hidden * lax.rsqrt(mean + 0.25)).astype(jnp.bfloat16)
            else:
                summed[k, rows, :] = total.astype(jnp.bfloat16)
            return 0

        lax.fori_loop(0, half // step, body, 0)

    def after(k):
        if k == NEAR:
            spreads[0].wait_recv()
            spreads[3].start()
            spreads[5].start()
            spreads[1].wait_recv()
            spreads[4].start()
            spreads[6].start()
        if k == FAR:
            spreads[3].wait_recv()
            spreads[7].start()
            spreads[4].wait_recv()
            spreads[8].start()
        for h in range(2):
            if CHILDREN[k]:
                form(k, h)
            if HOPS[k][1] is not None:
                hops[k, h].start()

    def block(k, _):
        compute(k)
        for i in range(len(HOPS)):
            pl.when(k == i)(functools.partial(after, i))
        return 0

    lax.fori_loop(0, len(HOPS), block, 0)
    for k in (2, 5, 6, 7, 8):
        spreads[k].wait_recv()

    tile = own_rows // 2

    def score(block, h):
        cols = slice(h * tile, h * tile + tile)
        scores = lax.dot_general(
            negative_ref[...], matrix[h, 0:tile, :], (((1,), (1,)), ((), ())),
            preferred_element_type=jnp.float32,
        )
        scores = 0.25 * scores - column_ref[...]
        peak = jnp.max(scores, axis=0, keepdims=True)
        partial[block, 0:1, cols] = peak
        partial[block, 1:2, cols] = jnp.sum(jnp.exp(scores - peak), axis=0, keepdims=True)

    def tile_load(i, h):
        rows = pl.ds(h * tile, tile)
        source = queries_ref.at[rows] if i is None else gathered.at[lax.rem(q + i, qrys), rows]
        return pltpu.make_async_copy(source, matrix.at[h, pl.ds(0, tile)], tile_sem.at[h])

    def tile_start(i, h):
        @pl.when(i < qrys)
        def _():
            tile_load(i, h).start()

        @pl.when(i == qrys)
        def _():
            tile_load(None, h).start()

    for h in range(2):
        tile_load(1, h).start()

    def first(i):
        to = lax.rem(q + i, qrys)
        return pltpu.make_async_remote_copy(
            src_ref=partial.at[to], dst_ref=first_in.at[i],
            send_sem=first_send.at[i], recv_sem=first_recv.at[i],
            device_id=(n, to), device_id_type=MESH,
        )

    def each(i, _):
        for h in range(2):
            tile_load(None, h).wait()
            score(lax.rem(q + i, qrys), h)
            tile_start(i + 1, h)

        @pl.when(i > 1)
        def _():
            first(i - 1).start()

        return 0

    lax.fori_loop(1, qrys + 1, each, 0)
    peak, total = partial[q, 0:1, :], partial[q, 1:2, :]
    for i in range(1, qrys):
        first(i).wait_recv()
        peak, total = join(peak, total, first_in[i, 0:1, :], first_in[i, 1:2, :])
    second_out[0:1, :] = peak
    second_out[1:2, :] = total

    def second(i):
        return pltpu.make_async_remote_copy(
            src_ref=second_out, dst_ref=second_in.at[i],
            send_sem=second_send.at[i], recv_sem=second_recv.at[i],
            device_id=(lax.rem(n + i, parts), q), device_id_type=MESH,
        )

    for i in range(1, parts):
        second(i).start()
    for k in range(len(HOPS) - 1):
        for h in range(2):
            hops[k, h].wait_send()
    for k in range(9):
        spreads[k].wait_send()
    for i in range(1, qrys):
        first(i).wait_send()
    for i in range(1, parts):
        second(i).wait_recv()
        peak, total = join(peak, total, second_in[i, 0:1, :], second_in[i, 1:2, :])
    lse_ref[...] = peak + jnp.log(total) - math.log(count * parts * qrys)
    for i in range(1, parts):
        second(i).wait_send()


def tower(words, counts, items, weights, bias, log_count, queries, qrys):
    parts, cap, count = counts.shape
    own_rows, width = queries.shape
    vmem = pl.BlockSpec(memory_space=pltpu.VMEM)
    smem = pl.BlockSpec(memory_space=pltpu.SMEM)
    hbm = pl.BlockSpec(memory_space=pltpu.HBM)
    dma = pltpu.SemaphoreType.DMA
    hops = len(HOPS) - 1
    return pl.pallas_call(
        functools.partial(tower_kernel, parts, qrys),
        in_specs=[smem, hbm, hbm, vmem, vmem, vmem, vmem, vmem, vmem, hbm],
        out_specs=(vmem, vmem, hbm),
        out_shape=(
            pltpu.VMEM((count, width), jnp.bfloat16),
            pltpu.VMEM((1, own_rows), jnp.float32),
            jax.ShapeDtypeStruct((qrys, own_rows, width), jnp.bfloat16),
        ),
        scratch_shapes=[
            pltpu.VMEM((4 * items.shape[0], 128), jnp.float32),
            pltpu.VMEM((4 * items.shape[0] + 8, 128), jnp.float32),
            pltpu.VMEM((2, 512, width), jnp.bfloat16),
            pltpu.VMEM((hops, count, width), jnp.bfloat16),
            pltpu.VMEM((hops + 1, count, width), jnp.bfloat16),
            pltpu.VMEM((2, cap, count), jnp.bfloat16),
            pltpu.VMEM((4 * cap, 128), jnp.float32),
            pltpu.VMEM((4 * count, 128), jnp.float32),
            pltpu.VMEM((count, 1), jnp.float32),
            pltpu.VMEM((qrys, 2, own_rows), jnp.float32),
            pltpu.VMEM((qrys, 2, own_rows), jnp.float32),
            pltpu.VMEM((2, own_rows), jnp.float32),
            pltpu.VMEM((parts, 2, own_rows), jnp.float32),
            dma((2,)), dma((2,)), dma((2,)), dma((hops, 2)), dma((hops, 2)), dma((9,)), dma((9,)),
            dma((qrys,)), dma((qrys,)), dma((parts,)), dma((parts,)),
        ],
        name="tower",
        compiler_params=pltpu.CompilerParams(
            collective_id=0, has_side_effects=True, vmem_limit_bytes=TOWER_VMEM
        ),
    )(words, counts, items, *weights, bias, log_count, queries)


def per_device(
    items_table,
    fetch_rows,
    neighbour_slots,
    neighbour_count,
    self_slot,
    negative_count,
    message_weight,
    message_bias,
    self_weight,
    neighbour_weight,
    output_bias,
    queries,
):
    parts, cap = fetch_rows.shape
    count, neighbours = neighbour_slots.shape

    assert items_table.shape[0] == ITEM_ROWS
    lists = [
        pltpu.with_memory_space_constraint(x, pltpu.HBM)
        for x in (neighbour_slots.T, neighbour_count[None], self_slot[None], fetch_rows)
    ]
    slab, words = prepare(*lists)
    slab, words = exchange(slab, words)
    words = words.reshape(-1)

    matrices = counts_blocks(words, slab, cap)
    matrices = pltpu.with_memory_space_constraint(matrices, pltpu.HBM)
    negative_embed, query_lse, _ = tower(
        words, matrices, items_table,
        (message_weight, message_bias[None], neighbour_weight, self_weight),
        output_bias[None], negative_count.reshape(-1, count), queries,
        lax.axis_size("qry"),
    )
    return (negative_embed, query_lse[0])


def solution(mesh):
    in_specs = (
        P("neg", None),
        P(("neg", "qry"), None),
        P(("neg", "qry"), None),
        P(("neg", "qry")),
        P(("neg", "qry")),
        P("neg"),
        P(),
        P(),
        P(),
        P(),
        P(),
        P("qry", None),
    )
    out_specs = (P(("neg", "qry"), None), P("qry"))
    return jax.shard_map(
        per_device, mesh=mesh, in_specs=in_specs, out_specs=out_specs, check_vma=False
    )
```
